512 devices in a mesh: obs: 16 (over x, y), patch: 32 (over z, core).
Axes of the slice: x: 4, y: 4, z: 16, core: 2. Of those that a mesh axis runs over, the one named last changes fastest.
Arguments:
- green: float32 [20480, 20480], P('obs', 'patch'), may hold values from -0.0390625 to 0.0390625
- data: float32 [20480, 128], P('obs'), may hold values from -6 to 6
- neighbours: int32 [3, 20480], P(None, 'patch'), may hold values from 0 to 20479, as said below
- reg_weight: float32 [128], replicated, may hold values from 0.5 to 2
Outputs:
- slip: float32 [20480, 128], P('patch')
The draws below stay inside these ranges and needn't reach their ends.
Inputs may be any that keep to these rules, and one draw needn't show every extreme that they name: `neighbours`: entry (k, i) is a patch within 128 of i; an entry equal to i is padding. Distance 128 is reached in every draw.
All inputs are finite; a program needn't handle non-finite values.
Results may differ from the reference program's by a relative error of at most 0.0001.
Values sent between devices are 32-bit elements; how exact they have to be, the bound alone decides.
No kernel may reach another device: no remote copies, remote signals or barrier semaphores. Data moves between devices by JAX's collectives and lax.ppermute only.
A program may use at most 64 MiB of HBM per device.

```python
import math
import jax
import jax.numpy as jnp
from jax import lax

EPOCHS = 128
BAND = 128
ITERS = 3
OBS = 20480
NPATCH = 20480


def draw_neighbours(key, part):
    key_offsets = jax.random.fold_in(key, 11)
    key_padding = jax.random.fold_in(key, 12)
    offsets = jax.random.randint(key_offsets, (3, NPATCH), -BAND, BAND + 1)
    padding = jax.random.randint(key_padding, (3, NPATCH), 0, 4) == 0
    offsets = jnp.where(padding, 0, offsets)
    indices = jnp.arange(NPATCH, dtype=jnp.int32)
    marked = indices % 37 == 5
    offsets = offsets.at[0].set(jnp.where(marked, -BAND, offsets[0]))
    offsets = offsets.at[1].set(jnp.where(marked, BAND, offsets[1]))
    return jnp.clip(indices[None, :] + offsets, 0, NPATCH - 1).astype(jnp.int32)


def level_of(key, extent, split, least, largest):
    level = 1.0
    for position, parts in split:
        draws = jax.random.uniform(jax.random.fold_in(jax.random.fold_in(key, 6), position), (parts,), jnp.float32, least / len(split), largest / len(split))
        level = level * jnp.repeat(jnp.exp(draws), extent[position] // parts).reshape((-1,) + (1,) * (len(extent) - 1 - position))
    return level


def gaussian(stream_key, dims, spread, most, shards=(), kind=jnp.bfloat16):
    loudness = level_of(stream_key, dims, shards, -0.22, 0.18) if shards else 1.0
    array = jax.random.normal(stream_key, dims, jnp.float32) * spread * loudness
    return jnp.minimum(jnp.maximum(array, -most), most).astype(kind)


def setup_inputs(seed: int = 0) -> dict:
    seeds = jax.random.split(jax.random.key(seed), 5)
    green = gaussian(seeds[0], (OBS, NPATCH), NPATCH ** -0.5, 0.0390625, ((0, 16), (1, 32)), jnp.float32)
    data = gaussian(seeds[1], (OBS, EPOCHS), 1.0, 6.0, ((0, 16),), jnp.float32)
    neighbours = draw_neighbours(jax.random.fold_in(seeds[4], 71), 0)
    reg_weight = jnp.clip(jnp.exp(jax.random.uniform(seeds[3], (EPOCHS,), jnp.float32, math.log(0.5), math.log(2.0))), 0.5, 2.0)
    return {"green": green, "data": data, "neighbours": neighbours, "reg_weight": reg_weight}


def laplace(field, neighbours):
    return 4.0 * field - field[neighbours[0]] - field[neighbours[1]] - field[neighbours[2]]


def laplace_t(values, neighbours):
    result = 4.0 * values
    for slot in range(3):
        result = result.at[neighbours[slot]].add(-values)
    return result


def transposed(green, residual):
    return lax.dot_general(green, residual, (((0,), (0,)), ((), ())), precision=lax.Precision.HIGHEST, preferred_element_type=jnp.float32)


def reference(green, data, neighbours, reg_weight):
    slip = jnp.zeros((NPATCH, EPOCHS), jnp.float32)
    residual = data
    reg_resid = jnp.zeros((NPATCH, EPOCHS), jnp.float32)
    gradient = transposed(green, data)
    grad_norm = jnp.sum(gradient * gradient, axis=0)
    direction = gradient
    for iteration in range(ITERS):
        image = jnp.dot(green, direction, precision=lax.Precision.HIGHEST, preferred_element_type=jnp.float32)
        reg_image = reg_weight * laplace(direction, neighbours)
        curvature = jnp.sum(image * image, axis=0) + jnp.sum(reg_image * reg_image, axis=0)
        step_size = grad_norm / curvature
        slip = slip + step_size * direction
        if iteration + 1 < ITERS:
            residual = residual - step_size * image
            reg_resid = reg_resid - step_size * reg_image
            gradient = transposed(green, residual) + reg_weight * laplace_t(reg_resid, neighbours)
            next_norm = jnp.sum(gradient * gradient, axis=0)
            direction = gradient + (next_norm / grad_norm) * direction
            grad_norm = next_norm
    return slip
```

```python
import jax
import jax.numpy as jnp
from jax import lax
from jax.sharding import Mesh
from jax.sharding import PartitionSpec as P

BAND = 128
ITERS = 3
OBS = ("x", "y")
PATCH = ("z", "c")
PREC = lax.Precision.HIGH
TILE = 8


def dot(a, b):
    return jnp.dot(a, b, precision=PREC, preferred_element_type=jnp.float32)


def dot_t(a, b):
    dims = (((0,), (0,)), ((), ()))
    return lax.dot_general(a, b, dims, precision=PREC, preferred_element_type=jnp.float32)


def total(x):
    return jnp.sum(x, axis=0, keepdims=True)


def rows_of(parts, epochs):
    pad = jnp.zeros((TILE - len(parts), epochs), jnp.float32)
    return jnp.concatenate([*parts, pad], 0)


def exchanged(pieces, axis):
    return lax.all_to_all(pieces, axis, 0, 0, tiled=True)


def broadcast(block, axis, count):
    return exchanged(jnp.broadcast_to(block[None], (count, *block.shape)), axis)


def to_neighbours(last, first, axis):
    count = lax.axis_size(axis)
    up = [(i, i + 1) for i in range(count - 1)]
    down = [(i + 1, i) for i in range(count - 1)]
    return lax.ppermute(last, axis, up), lax.ppermute(first, axis, down)


def laplace_square(neighbours, col_count, n_patch_blocks):
    block = lax.axis_index(PATCH)
    before, after = to_neighbours(neighbours[:, col_count - BAND :], neighbours[:, :BAND], PATCH)
    ids = jnp.concatenate([before, neighbours, after], 1) - (block * col_count - 2 * BAND)
    height, width = col_count + 2 * BAND, col_count + 4 * BAND
    row = lax.broadcasted_iota(jnp.int32, (height, width), 0)
    col = lax.broadcasted_iota(jnp.int32, (height, width), 1)
    entry = jnp.where(col == row + BAND, 4.0, 0.0)
    for slot in range(3):
        entry = entry - jnp.where(col == ids[slot][:, None], 1.0, 0.0)
    here = row + (block * col_count - BAND)
    inside = (here >= 0) & (here < col_count * n_patch_blocks)
    rows = jnp.where(inside, entry, 0.0).astype(jnp.bfloat16)
    own = rows[:, 2 * BAND : 2 * BAND + col_count]
    dims = (((0,), (0,)), ((), ()))
    return lax.dot_general(own, rows, dims, preferred_element_type=jnp.float32)


def shards(green, data, neighbours, reg_weight):
    row_count, col_count = green.shape
    epochs = data.shape[1]
    n_obs, n_z, n_core = lax.axis_size(OBS), lax.axis_size("z"), lax.axis_size("c")
    n_patch = n_z * n_core
    half = row_count // n_core
    core = lax.axis_index("c")
    share = row_count // n_patch
    piece = col_count // n_obs
    square = laplace_square(neighbours, col_count, n_patch)
    weight_sq = (reg_weight * reg_weight)[None]

    def image_share(field):
        partial = dot(green, field)
        keep = lax.dynamic_slice_in_dim(partial, core * half, half, 0)
        send = lax.dynamic_slice_in_dim(partial, (1 - core) * half, half, 0)
        other = lax.ppermute(send, "c", [(0, 1), (1, 0)])
        pieces = exchanged((keep + other).reshape(n_z, share, epochs), "z")
        return jnp.sum(pieces, axis=0)

    def over_patches(block, tail):
        every = lax.all_gather(jnp.concatenate([block, tail], 0), PATCH)
        image = every[:, :share].reshape(n_z, n_core, share, epochs)
        image = image.transpose(1, 0, 2, 3).reshape(row_count, epochs)
        return image, jnp.sum(every[:, share:], axis=0)

    def back(field, tail):
        partial = dot_t(green, field).reshape(n_obs, piece, epochs)
        part = jnp.sum(exchanged(partial, OBS), axis=0)
        every = broadcast(jnp.concatenate([part, tail], 0), OBS, n_obs)
        return every[:, :piece].reshape(col_count, epochs), jnp.sum(every[:, piece:], axis=0)

    def squared_laplace(field):
        before, after = to_neighbours(field[col_count - 2 * BAND :], field[: 2 * BAND], PATCH)
        return weight_sq * dot(square, jnp.concatenate([before, field, after], 0))

    gradient, _ = back(data, rows_of([], epochs))
    norm = image = smooth = direction = slip = None
    for iteration in range(ITERS):
        first, last = iteration == 0, iteration + 1 == ITERS
        part = image_share(gradient)
        fresh = squared_laplace(gradient)
        sums = [total(gradient * gradient), total(gradient * fresh)]
        if not first:
            sums.append(total(gradient * smooth))
        if last:
            place = (core * half + lax.axis_index("z") * share, 0)
            old = lax.dynamic_slice(image, place, (share, epochs))
            sums = [*sums, total(part * part), total(part * old)]
            tail = broadcast(rows_of(sums, epochs), OBS, n_obs)
            crossed = jnp.sum(tail, axis=0)
            tail = jnp.concatenate([tail[0, :3], crossed[3:]], 0)
            tail = jnp.sum(broadcast(tail, PATCH, n_patch), axis=0)
        else:
            new_image, tail = over_patches(part, rows_of(sums, epochs))
        new_norm = tail[0:1]
        if first:
            ratio = None
            direction, image, smooth = gradient, new_image, fresh
            reg_sq = tail[1:2]
        else:
            ratio = new_norm / norm
            reg_sq = tail[1:2] + ratio * (2.0 * tail[2:3] + ratio * reg_sq)
            direction = gradient + ratio * direction
            if not last:
                image = new_image + ratio * image
                smooth = fresh + ratio * smooth
        norm = new_norm
        if last:
            curvature = tail[3:4] + ratio * (2.0 * tail[4:5] + ratio * image_sq) + reg_sq
            return slip + norm / curvature * direction
        moved, tail = back(image, rows_of([total(image * image)], epochs))
        image_sq = tail[0:1]
        step = norm / (image_sq + reg_sq)
        slip = step * direction if first else slip + step * direction
        gradient = gradient - step * (moved + smooth)


def solution(mesh):
    split = Mesh(mesh.devices.reshape(4, 4, 16, 2), (*OBS, *PATCH))
    in_specs = (P(OBS, PATCH), P(OBS, None), P(None, PATCH), P())
    return jax.shard_map(
        shards, mesh=split, in_specs=in_specs, out_specs=P(PATCH, None), check_vma=False
    )
```

```python
import jax
import jax.numpy as jnp
from jax import lax
from jax.experimental import pallas as pl
from jax.experimental.pallas import tpu as pltpu
from jax.sharding import Mesh
from jax.sharding import PartitionSpec as P

BAND = 128
ITERS = 3
OBS = ("x", "y")
PATCH = ("z", "c")
TILE = 8
F32, BF16 = jnp.float32, jnp.bfloat16


def local_call(body, outs, *args, scalars=(), scratch=(), mib=24):
    vmem = pl.BlockSpec(memory_space=pltpu.VMEM)
    smem = pl.BlockSpec(memory_space=pltpu.SMEM)
    return pl.pallas_call(
        body,
        out_shape=[jax.ShapeDtypeStruct(shape, kind) for shape, kind in outs],
        in_specs=[smem] * len(scalars) + [vmem] * len(args),
        out_specs=[vmem] * len(outs),
        scratch_shapes=list(scratch),
        compiler_params=pltpu.CompilerParams(vmem_limit_bytes=mib << 20),
        name=body.__name__,
    )(*scalars, *args)


def halves(x):
    high = x.astype(BF16)
    return high, (x - high.astype(F32)).astype(BF16)


def store_halves(ref, start, x):
    high, low = halves(x)
    ref[start : start + x.shape[0], : x.shape[1]] = high
    ref[start : start + x.shape[0], x.shape[1] :] = low


def product(high_ref, low_ref, wide):
    width = wide.shape[1] // 2
    both = jnp.dot(high_ref[...], wide, preferred_element_type=F32)
    both = both + jnp.dot(low_ref[...], wide, preferred_element_type=F32)
    return both[:, :width] + both[:, width:]


def total(x):
    return jnp.sum(x, axis=0, keepdims=True)


def put_rows(ref, rows):
    ref[...] = jnp.zeros_like(ref)
    for place, row in enumerate(rows):
        ref[place : place + 1, :] = row


def summed(pieces_ref):
    value = pieces_ref[0]
    for k in range(1, pieces_ref.shape[0]):
        value = value + pieces_ref[k]
    return value


def first_back(green, data, high, low, moved, wide):
    for k in range(green.shape[0] // 128):
        high[:, 128 * k : 128 * (k + 1)], low[:, 128 * k : 128 * (k + 1)] = halves(
            green[128 * k : 128 * (k + 1), :].T
        )
    store_halves(wide, 0, data[...])
    moved[...] = product(high, low, wide[...])


def split_forward(keep, other, high, low):
    width = keep.shape[1]
    high[:, :width], low[:, :width] = halves(keep[...])
    high[:, width:], low[:, width:] = halves(other[...])


def split_square(square, high, low):
    high[...], low[...] = halves(square[...])


def forward(core, field, other, edge, weight_sq, smooth, f_high, f_low, m_high, m_low, part, fresh, sums, wide, near):
    rows, reach = field.shape[0], 2 * BAND
    own = field[...]
    store_halves(wide, 0, own)
    store_halves(wide, rows, other[...])
    part[...] = product(f_high, f_low, wide[...])
    is_first = core[0] == 0
    outer = edge[...]
    store_halves(near, 0, jnp.where(is_first, outer, other[rows - reach :, :]))
    store_halves(near, reach, own)
    store_halves(near, reach + rows, jnp.where(is_first, other[:reach, :], outer))
    new = weight_sq[...] * product(m_high, m_low, near[...])
    fresh[...] = new
    put_rows(sums, [total(own * own), total(own * new), total(own * smooth[...])])


def collect(pieces, sums, out):
    share = pieces.shape[1]
    out[:share, :] = summed(pieces)
    out[share:, :] = sums[...]


def backward(every, field, fresh, old_image, old_smooth, old_way, old_scalars, high, low, moved, image, tail, smooth, way, scalars, wide):
    count = every.shape[0]
    share = every.shape[1] - TILE
    sums = every[0, share:, :]
    for k in range(1, count):
        sums = sums + every[k, share:, :]
    norm = sums[0:1]
    has_old = old_scalars[2:3, :] > 0.0
    ratio = jnp.where(has_old, norm / old_scalars[0:1, :], 0.0)
    square = jnp.zeros((TILE, every.shape[2]), F32)
    for k in range(0, count, 2):
        rows = slice(share * k, share * (k + 2))
        piece = jnp.concatenate([every[k, :share, :], every[k + 1, :share, :]], 0)
        piece = piece + ratio * old_image[rows, :]
        image[rows, :] = piece
        store_halves(wide, share * k, piece)
        for t in range(2 * share // TILE):
            block = piece[TILE * t : TILE * (t + 1)]
            square = square + block * block
    moved[...] = product(high, low, wide[...])
    put_rows(tail, [total(square)])
    smooth[...] = fresh[...] + ratio * old_smooth[...]
    way[...] = field[...] + ratio * old_way[...]
    reg_sq = sums[1:2] + ratio * (2.0 * sums[2:3] + ratio * old_scalars[1:2, :])
    put_rows(scalars, [norm, reg_sq, jnp.ones_like(norm)])


def spread(pieces, tail, out):
    share = pieces.shape[1]
    value, last = summed(pieces), tail[...]
    for k in range(out.shape[0]):
        out[k, :share, :] = value
        out[k, share:, :] = last


def start_field(every, field):
    share = every.shape[1] - TILE
    for k in range(every.shape[0]):
        field[share * k : share * (k + 1), :] = every[k, :share, :]


def update(every, scalars, smooth, way, old_field, old_slip, field, slip, kept):
    count = every.shape[0]
    share = every.shape[1] - TILE
    image_sq = every[0, share : share + 1, :]
    for k in range(1, count):
        image_sq = image_sq + every[k, share : share + 1, :]
    step = scalars[0:1, :] / (image_sq + scalars[1:2, :])
    for k in range(count):
        rows = slice(share * k, share * (k + 1))
        field[rows, :] = old_field[rows, :] - step * (every[k, :share, :] + smooth[rows, :])
    slip[...] = old_slip[...] + step * way[...]
    put_rows(kept, [scalars[0:1, :], scalars[1:2, :], scalars[2:3, :], image_sq])


def last_sums(place, pieces, image, sums, out):
    share = pieces.shape[1]
    part = summed(pieces)
    start = pl.multiple_of(place[0] * share, TILE)
    old = image[pl.ds(start, share), :]
    new = total(part * part)
    cross = total(part * old)
    for k in range(out.shape[0]):
        out[k] = sums[...]
        out[k, 3:4, :] = new
        out[k, 4:5, :] = cross


def last_spread(every, out):
    sums = summed(every)
    for k in range(out.shape[0]):
        out[k] = sums
        out[k, 0:3, :] = every[0, 0:3, :]


def last_update(every, kept, field, way, old_slip, slip):
    sums = summed(every)
    norm, old_norm, reg_sq, image_sq = sums[0:1], kept[0:1, :], kept[1:2, :], kept[3:4, :]
    ratio = norm / old_norm
    reg_sq = sums[1:2] + ratio * (2.0 * sums[2:3] + ratio * reg_sq)
    image_sq = sums[3:4] + ratio * (2.0 * sums[4:5] + ratio * image_sq)
    step = norm / (image_sq + reg_sq)
    slip[...] = old_slip[...] + step * (field[...] + ratio * way[...])


def to_neighbours(last, first, axis):
    count = lax.axis_size(axis)
    up = [(i, i + 1) for i in range(count - 1)]
    down = [(i + 1, i) for i in range(count - 1)]
    return lax.ppermute(last, axis, up), lax.ppermute(first, axis, down)


def laplace_square(neighbours, col_count, n_patch_blocks):
    block = lax.axis_index(PATCH)
    before, after = to_neighbours(neighbours[:, col_count - BAND :], neighbours[:, :BAND], PATCH)
    ids = jnp.concatenate([before, neighbours, after], 1) - (block * col_count - 2 * BAND)
    height, width = col_count + 2 * BAND, col_count + 4 * BAND
    row = lax.broadcasted_iota(jnp.int32, (height, width), 0)
    col = lax.broadcasted_iota(jnp.int32, (height, width), 1)
    entry = jnp.where(col == row + BAND, 4.0, 0.0)
    for slot in range(3):
        entry = entry - jnp.where(col == ids[slot][:, None], 1.0, 0.0)
    here = row + (block * col_count - BAND)
    inside = (here >= 0) & (here < col_count * n_patch_blocks)
    rows = jnp.where(inside, entry, 0.0).astype(BF16)
    own = rows[:, 2 * BAND : 2 * BAND + col_count]
    dims = (((0,), (0,)), ((), ()))
    return lax.dot_general(own, rows, dims, preferred_element_type=F32)


def exchanged(pieces, axis):
    return lax.all_to_all(pieces, axis, 0, 0, tiled=True)


def shards(green, data, neighbours, reg_weight):
    row_count, col_count = green.shape
    epochs = data.shape[1]
    n_obs, n_z, n_core = lax.axis_size(OBS), lax.axis_size("z"), lax.axis_size("c")
    n_patch = n_z * n_core
    core = lax.axis_index("c")
    share = row_count // n_patch
    piece = col_count // n_obs
    half = row_count // n_core
    weight_sq = (reg_weight * reg_weight)[None]
    core_scalar = core.astype(jnp.int32)[None]
    place_scalar = lax.axis_index(PATCH).astype(jnp.int32)[None]
    swap = [(0, 1), (1, 0)]
    outward = [(2 * z + 1, 2 * z + 2) for z in range(n_z - 1)]
    outward = outward + [(b, a) for a, b in outward]

    field_shape = ((col_count, epochs), F32)
    image_shape = ((row_count, epochs), F32)
    tail_shape = ((TILE, epochs), F32)
    wide = pltpu.VMEM((row_count, 2 * epochs), BF16)

    matrix = ((col_count, row_count), BF16)
    b_high, b_low, moved = local_call(
        first_back, [matrix, matrix, field_shape], green, data, scratch=[wide]
    )
    pieces = exchanged(moved.reshape(n_obs, piece, epochs), OBS)

    by_core = green.reshape(n_z, n_core, share, col_count)
    keep = lax.dynamic_index_in_dim(by_core, core, 1, False).reshape(half, col_count)
    send = lax.dynamic_index_in_dim(by_core, 1 - core, 1, False).reshape(half, col_count)
    matrix = ((half, n_core * col_count), BF16)
    f_high, f_low = local_call(split_forward, [matrix, matrix], keep, lax.ppermute(send, "c", swap))
    square = laplace_square(neighbours, col_count, n_patch)
    matrix = (square.shape, BF16)
    m_high, m_low = local_call(split_square, [matrix, matrix], square)

    zero_tail = jnp.zeros((TILE, epochs), F32)
    zero_field = jnp.zeros((col_count, epochs), F32)
    spread_shape = ((n_obs, piece + TILE, epochs), F32)
    (out,) = local_call(spread, [spread_shape], pieces, zero_tail)
    (field,) = local_call(start_field, [field_shape], exchanged(out, OBS))

    kept, slip, smooth, way = zero_tail, zero_field, zero_field, zero_field
    image = jnp.zeros((row_count, epochs), F32)
    for iteration in range(ITERS):
        other = lax.ppermute(field, "c", swap)
        reach = 2 * BAND
        edge = jnp.where(core == 0, field[:reach], field[col_count - reach :])
        edge = lax.ppermute(edge, PATCH, outward)
        near = pltpu.VMEM((col_count + 2 * reach, 2 * epochs), BF16)
        part, fresh, sums = local_call(
            forward,
            [((half, epochs), F32), field_shape, tail_shape],
            field, other, edge, weight_sq, smooth, f_high, f_low, m_high, m_low,
            scalars=[core_scalar],
            scratch=[wide, near],
        )
        pieces = exchanged(part.reshape(n_z, share, epochs), "z")
        if iteration + 1 == ITERS:
            shape = ((n_obs, TILE, epochs), F32)
            (out,) = local_call(last_sums, [shape], pieces, image, sums, scalars=[place_scalar])
            shape = ((n_patch, TILE, epochs), F32)
            (out,) = local_call(last_spread, [shape], exchanged(out, OBS))
            (slip,) = local_call(
                last_update, [field_shape], exchanged(out, PATCH), kept, field, way, slip
            )
            return slip
        (out,) = local_call(collect, [((share + TILE, epochs), F32)], pieces, sums)
        every = lax.all_gather(out, PATCH)
        moved, image, tail, smooth, way, scalars = local_call(
            backward,
            [field_shape, image_shape, tail_shape, field_shape, field_shape, tail_shape],
            every, field, fresh, image, smooth, way, kept, b_high, b_low,
            scratch=[wide],
        )
        pieces = exchanged(moved.reshape(n_obs, piece, epochs), OBS)
        (out,) = local_call(spread, [spread_shape], pieces, tail)
        field, slip, kept = local_call(
            update, [field_shape, field_shape, tail_shape],
            exchanged(out, OBS), scalars, smooth, way, field, slip,
        )


def solution(mesh):
    split = Mesh(mesh.devices.reshape(4, 4, 16, 2), (*OBS, *PATCH))
    in_specs = (P(OBS, PATCH), P(OBS, None), P(None, PATCH), P())
    return jax.shard_map(
        shards, mesh=split, in_specs=in_specs, out_specs=P(PATCH, None), check_vma=False
    )
```

```python
import functools

import jax
import jax.numpy as jnp
from jax import lax
from jax.experimental import pallas as pl
from jax.experimental.pallas import tpu as pltpu
from jax.sharding import Mesh
from jax.sharding import PartitionSpec as P

BAND = 128
ITERS = 3
OBS = ("x", "y")
PATCH = ("z", "c")
TILE = 8
F32, BF16 = jnp.float32, jnp.bfloat16


def local_call(body, outs, *args, scalars=(), scratch=(), mib=24, **options):
    vmem = pl.BlockSpec(memory_space=pltpu.VMEM)
    smem = pl.BlockSpec(memory_space=pltpu.SMEM)
    return pl.pallas_call(
        functools.partial(body, **options),
        out_shape=[jax.ShapeDtypeStruct(shape, kind) for shape, kind in outs],
        in_specs=[smem] * len(scalars) + [vmem] * len(args),
        out_specs=[vmem] * len(outs),
        scratch_shapes=list(scratch),
        compiler_params=pltpu.CompilerParams(vmem_limit_bytes=mib << 20),
    )(*scalars, *args)


def halves(x):
    high = x.astype(BF16)
    return high, (x - high.astype(F32)).astype(BF16)


def store_halves(ref, start, x):
    high, low = halves(x)
    ref[start : start + x.shape[0], : x.shape[1]] = high
    ref[start : start + x.shape[0], x.shape[1] :] = low


def product(high_ref, low_ref, wide):
    width = wide.shape[1] // 2
    both = jnp.dot(high_ref[...], wide, preferred_element_type=F32)
    both = both + jnp.dot(low_ref[...], wide, preferred_element_type=F32)
    return both[:, :width] + both[:, width:]


def total(x):
    return jnp.sum(x, axis=0, keepdims=True)


def put_rows(ref, rows):
    ref[...] = jnp.zeros_like(ref)
    for place, row in enumerate(rows):
        ref[place : place + 1, :] = row


def summed(pieces_ref):
    value = pieces_ref[0]
    for k in range(1, pieces_ref.shape[0]):
        value = value + pieces_ref[k]
    return value


def turned(green, high, low):
    for k in range(green.shape[0] // 128):
        high[:, 128 * k : 128 * (k + 1)], low[:, 128 * k : 128 * (k + 1)] = halves(
            green[128 * k : 128 * (k + 1), :].T
        )


def first_back(green, data, moved, high, low, wide):
    turned(green, high, low)
    store_halves(wide, 0, data[...])
    moved[...] = product(high, low, wide[...])


def pick(core, green, ids, moved, send, last_ids, first_ids, *, share):
    last_ids[...] = ids[:, ids.shape[1] - BAND :]
    first_ids[...] = ids[:, :BAND]
    for k in range(send.shape[0] // share):
        theirs = pl.multiple_of((2 * k + 1 - core[0]) * share, TILE)
        send[share * k : share * (k + 1), :] = green[pl.ds(theirs, share), :]


def prepare(core, green, other, back_high, back_low, high, low, far_high, far_low, *, share):
    for z in range(0, high.shape[0] // share, 2):
        mine = [
            green[pl.ds(pl.multiple_of((2 * k + core[0]) * share, TILE), share), :]
            for k in (z, z + 1)
        ]
        rows = slice(share * z, share * (z + 2))
        high[rows, :], low[rows, :] = halves(jnp.concatenate(mine, 0))
    far_high[...], far_low[...] = halves(other[...])
    turned(green, back_high, back_low)


def laplace_square(block, before, ids, after, high, low, rows, own, ids_col):
    col_count = ids.shape[1]
    height, width = rows.shape
    total_cols = block[1] * col_count
    start = block[0] * col_count
    relative = jnp.concatenate([before[...], ids[...], after[...]], 1) - (start - 2 * BAND)
    pad = jnp.zeros((TILE - 3, height), jnp.int32)
    ids_col[...] = jnp.concatenate([relative, pad], 0).T
    here = lax.broadcasted_iota(jnp.int32, (1, height), 1) + (start - BAND)
    inside = jnp.where((here >= 0) & (here < total_cols), 1.0, 0.0)

    def fill_rows(i, carry):
        at = pl.multiple_of(i * 128, 128)
        row = lax.broadcasted_iota(jnp.int32, (128, width), 0) + at
        col = lax.broadcasted_iota(jnp.int32, (128, width), 1)
        entry = jnp.where(col == row + BAND, 4.0, 0.0)
        for slot in range(3):
            entry = entry - jnp.where(col == ids_col[pl.ds(at, 128), slot : slot + 1], 1.0, 0.0)
        rows[pl.ds(at, 128), :] = entry.astype(BF16)
        return carry

    lax.fori_loop(0, height // 128, fill_rows, 0)

    def fill_out(i, carry):
        at = pl.multiple_of(i * 128, 128)
        col = lax.broadcasted_iota(jnp.int32, (128, height), 0) + at
        row = lax.broadcasted_iota(jnp.int32, (128, height), 1)
        entry = jnp.where(row == col + BAND, 4.0, 0.0)
        for slot in range(3):
            entry = entry - jnp.where(col + 2 * BAND == relative[slot : slot + 1, :], 1.0, 0.0)
        own[...] = (entry * inside).astype(BF16)
        square = jnp.dot(own[...], rows[...], preferred_element_type=F32)
        high[pl.ds(at, 128), :], low[pl.ds(at, 128), :] = halves(square)
        return carry

    lax.fori_loop(0, col_count // 128, fill_out, 0)


def forward(core, field, other, edge, weight_sq, smooth, own_high, own_low, far_high, far_low, m_high, m_low, part, sums, fresh, wide, near):
    rows, reach = field.shape[0], 2 * BAND
    own = field[...]
    store_halves(wide, 0, own)
    store_halves(wide, rows, other[...])
    part[...] = product(own_high, own_low, wide[:rows, :]) + product(far_high, far_low, wide[rows:, :])
    is_first = core[0] == 0
    outer = edge[...]
    store_halves(near, 0, jnp.where(is_first, outer, other[rows - reach :, :]))
    store_halves(near, reach, own)
    store_halves(near, reach + rows, jnp.where(is_first, other[:reach, :], outer))
    new = weight_sq[...] * product(m_high, m_low, near[...])
    fresh[...] = new
    put_rows(sums, [total(own * own), total(own * new), total(own * smooth[...])])


def collect(pieces, sums, out):
    share = pieces.shape[1]
    out[:share, :] = summed(pieces)
    out[share:, :] = sums[...]


def backward(every, field, fresh, old_image, old_smooth, old_way, old_scalars, high, low, moved, image, tail, smooth, way, scalars, wide):
    count = every.shape[0]
    share = every.shape[1] - TILE
    sums = every[0, share:, :]
    for k in range(1, count):
        sums = sums + every[k, share:, :]
    norm = sums[0:1]
    has_old = old_scalars[2:3, :] > 0.0
    ratio = jnp.where(has_old, norm / old_scalars[0:1, :], 0.0)
    square = jnp.zeros((TILE, every.shape[2]), F32)
    for k in range(0, count, 2):
        rows = slice(share * k, share * (k + 2))
        piece = jnp.concatenate([every[k, :share, :], every[k + 1, :share, :]], 0)
        piece = piece + ratio * old_image[rows, :]
        image[rows, :] = piece
        store_halves(wide, share * k, piece)
        for t in range(2 * share // TILE):
            block = piece[TILE * t : TILE * (t + 1)]
            square = square + block * block
    moved[...] = product(high, low, wide[...])
    put_rows(tail, [total(square)])
    smooth[...] = fresh[...] + ratio * old_smooth[...]
    way[...] = field[...] + ratio * old_way[...]
    reg_sq = sums[1:2] + ratio * (2.0 * sums[2:3] + ratio * old_scalars[1:2, :])
    put_rows(scalars, [norm, reg_sq, jnp.ones_like(norm)])


def spread(pieces, tail, out):
    share = pieces.shape[1]
    value, last = summed(pieces), tail[...]
    for k in range(out.shape[0]):
        out[k, :share, :] = value
        out[k, share:, :] = last


def start_field(every, m_high, far_high, field):
    share = every.shape[1] - TILE
    for k in range(every.shape[0]):
        field[share * k : share * (k + 1), :] = every[k, :share, :]


def update(every, scalars, smooth, way, old_field, old_slip, field, slip, kept):
    count = every.shape[0]
    share = every.shape[1] - TILE
    image_sq = every[0, share : share + 1, :]
    for k in range(1, count):
        image_sq = image_sq + every[k, share : share + 1, :]
    step = scalars[0:1, :] / (image_sq + scalars[1:2, :])
    for k in range(count):
        rows = slice(share * k, share * (k + 1))
        field[rows, :] = old_field[rows, :] - step * (every[k, :share, :] + smooth[rows, :])
    slip[...] = old_slip[...] + step * way[...]
    put_rows(kept, [scalars[0:1, :], scalars[1:2, :], scalars[2:3, :], image_sq])


def last_sums(place, pieces, image, sums, out):
    share = pieces.shape[1]
    part = summed(pieces)
    start = pl.multiple_of(place[0] * share, TILE)
    old = image[pl.ds(start, share), :]
    first = jnp.concatenate([sums[0:3, :], total(part * part), total(part * old), sums[5:, :]], 0)
    for k in range(out.shape[0]):
        out[k] = first


def last_spread(every, out):
    sums, pair = summed(every), every[0] + every[1]
    first = jnp.concatenate([pair[0:3], sums[3:]], 0)
    for k in range(out.shape[0]):
        out[k] = first


def last_update(every, kept, field, way, old_slip, slip):
    sums = summed(every)
    norm, old_norm, reg_sq, image_sq = sums[0:1], kept[0:1, :], kept[1:2, :], kept[3:4, :]
    ratio = norm / old_norm
    reg_sq = sums[1:2] + ratio * (2.0 * sums[2:3] + ratio * reg_sq)
    image_sq = sums[3:4] + ratio * (2.0 * sums[4:5] + ratio * image_sq)
    step = norm / (image_sq + reg_sq)
    slip[...] = old_slip[...] + step * (field[...] + ratio * way[...])


def to_neighbours(last, first, axis):
    count = lax.axis_size(axis)
    up = [(i, i + 1) for i in range(count - 1)]
    down = [(i + 1, i) for i in range(count - 1)]
    return lax.ppermute(last, axis, up), lax.ppermute(first, axis, down)


def exchanged(pieces, axis):
    return lax.all_to_all(pieces, axis, 0, 0, tiled=True)


def shards(green, data, neighbours, reg_weight):
    row_count, col_count = green.shape
    epochs = data.shape[1]
    n_obs, n_z, n_core = lax.axis_size(OBS), lax.axis_size("z"), lax.axis_size("c")
    n_patch = n_z * n_core
    core = lax.axis_index("c")
    piece = col_count // n_obs
    half = row_count // n_core
    reach = 2 * BAND
    weight_sq = (reg_weight * reg_weight)[None]
    share = row_count // n_patch
    core_scalar = core.astype(jnp.int32)[None]
    place_scalar = lax.axis_index(PATCH).astype(jnp.int32)[None]
    block_scalars = jnp.stack([lax.axis_index(PATCH).astype(jnp.int32), jnp.int32(n_patch)])
    swap = [(0, 1), (1, 0)]
    outward = [(2 * z + 1, 2 * z + 2) for z in range(n_z - 1)]
    outward = outward + [(b, a) for a, b in outward]

    field_shape = ((col_count, epochs), F32)
    image_shape = ((row_count, epochs), F32)
    tail_shape = ((TILE, epochs), F32)
    wide = pltpu.VMEM((row_count, 2 * epochs), BF16)
    near = pltpu.VMEM((col_count + 2 * reach, 2 * epochs), BF16)

    back_matrix = ((col_count, row_count), BF16)
    (moved,) = local_call(
        first_back, [field_shape], green, data,
        scratch=[pltpu.VMEM(*back_matrix), pltpu.VMEM(*back_matrix), wide],
    )
    pieces = exchanged(moved.reshape(n_obs, piece, epochs), OBS)
    matrix = ((half, col_count), BF16)
    ids_shape = ((3, BAND), jnp.int32)
    send, last_ids, first_ids = local_call(
        pick, [((half, col_count), F32), ids_shape, ids_shape],
        green, neighbours, moved, scalars=[core_scalar], share=share,
    )
    far = lax.ppermute(send, "c", swap)
    before, after = to_neighbours(last_ids, first_ids, PATCH)

    zero_tail = jnp.zeros((TILE, epochs), F32)
    zero_field = jnp.zeros((col_count, epochs), F32)
    spread_shape = ((n_obs, piece + TILE, epochs), F32)
    (out,) = local_call(spread, [spread_shape], pieces, zero_tail)
    every = exchanged(out, OBS)
    b_high, b_low, own_high, own_low, far_high, far_low = local_call(
        prepare, [back_matrix, back_matrix, matrix, matrix, matrix, matrix],
        green, far, scalars=[core_scalar], share=share,
    )
    height, width = col_count + 2 * BAND, col_count + 4 * BAND
    m_matrix = ((col_count, width), BF16)
    m_high, m_low = local_call(
        laplace_square, [m_matrix, m_matrix], before, neighbours, after,
        scalars=[block_scalars],
        scratch=[
            pltpu.VMEM((height, width), BF16),
            pltpu.VMEM((128, height), BF16),
            pltpu.VMEM((height, TILE), jnp.int32),
        ],
    )
    (field,) = local_call(start_field, [field_shape], every, m_high, far_high)

    kept, slip, smooth, way = zero_tail, zero_field, zero_field, zero_field
    image = jnp.zeros((row_count, epochs), F32)
    for iteration in range(ITERS):
        other = lax.ppermute(field, "c", swap)
        edge = jnp.where(core == 0, field[:reach], field[col_count - reach :])
        edge = lax.ppermute(edge, PATCH, outward)
        part, sums, fresh = local_call(
            forward, [((half, epochs), F32), tail_shape, field_shape],
            field, other, edge, weight_sq, smooth,
            own_high, own_low, far_high, far_low, m_high, m_low,
            scalars=[core_scalar],
            scratch=[wide, near],
        )
        pieces = exchanged(part.reshape(n_z, share, epochs), "z")
        if iteration + 1 == ITERS:
            shape = ((n_obs * n_core, TILE, epochs), F32)
            (out,) = local_call(last_sums, [shape], pieces, image, sums, scalars=[place_scalar])
            every = exchanged(out, (*OBS, "c"))
            (out,) = local_call(last_spread, [((n_z, TILE, epochs), F32)], every)
            (slip,) = local_call(
                last_update, [field_shape], exchanged(out, "z"), kept, field, way, slip
            )
            return slip
        (out,) = local_call(collect, [((share + TILE, epochs), F32)], pieces, sums)
        every = lax.all_gather(out, PATCH)
        moved, image, tail, smooth, way, scalars = local_call(
            backward,
            [field_shape, image_shape, tail_shape, field_shape, field_shape, tail_shape],
            every, field, fresh, image, smooth, way, kept, b_high, b_low,
            scratch=[wide],
        )
        pieces = exchanged(moved.reshape(n_obs, piece, epochs), OBS)
        (out,) = local_call(spread, [spread_shape], pieces, tail)
        field, slip, kept = local_call(
            update, [field_shape, field_shape, tail_shape],
            exchanged(out, OBS), scalars, smooth, way, field, slip,
        )


def solution(mesh):
    split = Mesh(mesh.devices.reshape(4, 4, 16, 2), (*OBS, *PATCH))
    in_specs = (P(OBS, PATCH), P(OBS, None), P(None, PATCH), P())

    return jax.shard_map(
        shards, mesh=split, in_specs=in_specs, out_specs=P(PATCH, None), check_vma=False
    )
```

```python
import functools

import jax
import jax.numpy as jnp
from jax import lax
from jax.experimental import pallas as pl
from jax.experimental.pallas import tpu as pltpu
from jax.sharding import Mesh
from jax.sharding import PartitionSpec as P

BAND = 128
ITERS = 3
OBS = ("x", "y")
PATCH = ("z", "c")
TILE = 8
F32, BF16 = jnp.float32, jnp.bfloat16


def local_call(body, outs, *args, scalars=(), scratch=(), mib=24, **options):
    vmem = pl.BlockSpec(memory_space=pltpu.VMEM)
    smem = pl.BlockSpec(memory_space=pltpu.SMEM)
    return pl.pallas_call(
        functools.partial(body, **options),
        out_shape=[jax.ShapeDtypeStruct(shape, kind) for shape, kind in outs],
        in_specs=[smem] * len(scalars) + [vmem] * len(args),
        out_specs=[vmem] * len(outs),
        scratch_shapes=list(scratch),
        compiler_params=pltpu.CompilerParams(vmem_limit_bytes=mib << 20),
        name=body.__name__,
    )(*scalars, *args)


def halves(x):
    high = x.astype(BF16)
    return high, (x - high.astype(F32)).astype(BF16)


def store_halves(ref, start, x):
    high, low = halves(x)
    ref[start : start + x.shape[0], : x.shape[1]] = high
    ref[start : start + x.shape[0], x.shape[1] :] = low


def product(high_ref, low_ref, wide):
    width = wide.shape[1] // 2
    both = jnp.dot(high_ref[...], wide, preferred_element_type=F32)
    both = both + jnp.dot(low_ref[...], wide, preferred_element_type=F32)
    return both[:, :width] + both[:, width:]


def total(x):
    return jnp.sum(x, axis=0, keepdims=True)


def put_rows(ref, rows):
    ref[...] = jnp.zeros_like(ref)
    for place, row in enumerate(rows):
        ref[place : place + 1, :] = row


def summed(pieces_ref):
    value = pieces_ref[0]
    for k in range(1, pieces_ref.shape[0]):
        value = value + pieces_ref[k]
    return value


def first_back(core, green, data, moved, back_high, back_low, high, low, send, wide, *, share):
    for k in range(green.shape[0] // 128):
        at = slice(128 * k, 128 * (k + 1))
        back_high[:, at], back_low[:, at] = halves(green[at, :].T)
    store_halves(wide, 0, data[...])
    moved[...] = product(back_high, back_low, wide[...])
    for z in range(0, send.shape[0] // share, 2):
        mine = []
        for k in (z, z + 1):
            start = pl.multiple_of((2 * k + core[0]) * share, TILE)
            mine.append(green[pl.ds(start, share), :])
            start = pl.multiple_of((2 * k + 1 - core[0]) * share, TILE)
            send[share * k : share * (k + 1), :] = green[pl.ds(start, share), :]
        rows = slice(share * z, share * (z + 2))
        high[rows, :], low[rows, :] = halves(jnp.concatenate(mine, 0))


def split_other(other, high, low):
    high[...], low[...] = halves(other[...])


def laplace_square(block, before, ids, after, high, low, rows, own, ids_col):
    col_count = ids.shape[1]
    height = rows.shape[0]
    total_cols = block[1] * col_count
    start = block[0] * col_count
    relative = jnp.concatenate([before[...], ids[...], after[...]], 1) - (start - 2 * BAND)
    pad = jnp.zeros((TILE - 3, height), jnp.int32)
    ids_col[...] = jnp.concatenate([relative, pad], 0).T
    here = lax.broadcasted_iota(jnp.int32, (1, height), 1) + (start - BAND)
    inside = jnp.where((here >= 0) & (here < total_cols), 1.0, 0.0)
    rows[...] = jnp.zeros_like(rows)
    wide = 128 + 2 * BAND
    for i in range(height // 128):
        at = 128 * i
        row = lax.broadcasted_iota(jnp.int32, (128, wide), 0) + at
        col = lax.broadcasted_iota(jnp.int32, (128, wide), 1) + at
        entry = jnp.where(col == row + BAND, 4.0, 0.0)
        for slot in range(3):
            entry = entry - jnp.where(col == ids_col[at : at + 128, slot : slot + 1], 1.0, 0.0)
        rows[at : at + 128, at : at + wide] = entry.astype(BF16)
    high[...] = jnp.zeros_like(high)
    low[...] = jnp.zeros_like(low)
    for i in range(col_count // 128):
        at = 128 * i
        col = lax.broadcasted_iota(jnp.int32, (128, wide), 0) + at
        row = lax.broadcasted_iota(jnp.int32, (128, wide), 1) + at
        entry = jnp.where(row == col + BAND, 4.0, 0.0)
        for slot in range(3):
            target = relative[slot : slot + 1, at : at + wide]
            entry = entry - jnp.where(col + 2 * BAND == target, 1.0, 0.0)
        own[...] = (entry * inside[:, at : at + wide]).astype(BF16)
        reach = slice(at, at + 128 + 4 * BAND)
        square = jnp.dot(own[...], rows[at : at + wide, reach], preferred_element_type=F32)
        high[at : at + 128, reach], low[at : at + 128, reach] = halves(square)


def forward(core, field, other, edge, weight_sq, smooth, own_high, own_low, far_high, far_low, m_high, m_low, part, sums, fresh, wide, near):
    rows, reach = field.shape[0], 2 * BAND
    own = field[...]
    store_halves(wide, 0, own)
    store_halves(wide, rows, other[...])
    part[...] = product(own_high, own_low, wide[:rows, :]) + product(far_high, far_low, wide[rows:, :])
    is_first = core[0] == 0
    outer = edge[...]
    store_halves(near, 0, jnp.where(is_first, outer, other[rows - reach :, :]))
    store_halves(near, reach, own)
    store_halves(near, reach + rows, jnp.where(is_first, other[:reach, :], outer))
    new = weight_sq[...] * product(m_high, m_low, near[...])
    fresh[...] = new
    put_rows(sums, [total(own * own), total(own * new), total(own * smooth[...])])


def collect(pieces, sums, out):
    share = pieces.shape[1]
    out[:share, :] = summed(pieces)
    out[share:, :] = sums[...]


def backward(every, field, fresh, old_image, old_smooth, old_way, old_scalars, high, low, moved, image, tail, smooth, way, scalars, wide):
    count = every.shape[0]
    share = every.shape[1] - TILE
    sums = every[0, share:, :]
    for k in range(1, count):
        sums = sums + every[k, share:, :]
    norm = sums[0:1]
    has_old = old_scalars[2:3, :] > 0.0
    ratio = jnp.where(has_old, norm / old_scalars[0:1, :], 0.0)
    square = jnp.zeros((TILE, every.shape[2]), F32)
    for k in range(0, count, 2):
        rows = slice(share * k, share * (k + 2))
        piece = jnp.concatenate([every[k, :share, :], every[k + 1, :share, :]], 0)
        piece = piece + ratio * old_image[rows, :]
        image[rows, :] = piece
        store_halves(wide, share * k, piece)
        for t in range(2 * share // TILE):
            block = piece[TILE * t : TILE * (t + 1)]
            square = square + block * block
    moved[...] = product(high, low, wide[...])
    put_rows(tail, [total(square)])
    smooth[...] = fresh[...] + ratio * old_smooth[...]
    way[...] = field[...] + ratio * old_way[...]
    reg_sq = sums[1:2] + ratio * (2.0 * sums[2:3] + ratio * old_scalars[1:2, :])
    put_rows(scalars, [norm, reg_sq, jnp.ones_like(norm)])


def spread(pieces, tail, out):
    share = pieces.shape[1]
    value, last = summed(pieces), tail[...]
    for k in range(out.shape[0]):
        out[k, :share, :] = value
        out[k, share:, :] = last


def put_edge(core, field, edge):
    reach = edge.shape[0]
    edge[...] = jnp.where(core[0] == 0, field[:reach, :], field[field.shape[0] - reach :, :])


def start_field(core, every, ids, field, edge, last_ids, first_ids):
    last_ids[...] = ids[:, ids.shape[1] - BAND :]
    first_ids[...] = ids[:, :BAND]
    share = every.shape[1] - TILE
    for k in range(every.shape[0]):
        field[share * k : share * (k + 1), :] = every[k, :share, :]
    put_edge(core, field, edge)


def update(core, every, scalars, smooth, way, old_field, old_slip, field, edge, slip, kept):
    count = every.shape[0]
    share = every.shape[1] - TILE
    image_sq = every[0, share : share + 1, :]
    for k in range(1, count):
        image_sq = image_sq + every[k, share : share + 1, :]
    step = scalars[0:1, :] / (image_sq + scalars[1:2, :])
    for k in range(count):
        rows = slice(share * k, share * (k + 1))
        field[rows, :] = old_field[rows, :] - step * (every[k, :share, :] + smooth[rows, :])
    put_edge(core, field, edge)
    slip[...] = old_slip[...] + step * way[...]
    put_rows(kept, [scalars[0:1, :], scalars[1:2, :], scalars[2:3, :], image_sq])


def last_sums(place, pieces, image, sums, out):
    share = pieces.shape[1]
    part = summed(pieces)
    start = pl.multiple_of(place[0] * share, TILE)
    old = image[pl.ds(start, share), :]
    first = jnp.concatenate([sums[0:3, :], total(part * part), total(part * old), sums[5:, :]], 0)
    for k in range(out.shape[0]):
        out[k] = first


def last_spread(every, out):
    sums, pair = summed(every), every[0] + every[1]
    first = jnp.concatenate([pair[0:3], sums[3:]], 0)
    for k in range(out.shape[0]):
        out[k] = first


def last_update(every, kept, field, way, old_slip, slip):
    sums = summed(every)
    norm, old_norm, reg_sq, image_sq = sums[0:1], kept[0:1, :], kept[1:2, :], kept[3:4, :]
    ratio = norm / old_norm
    reg_sq = sums[1:2] + ratio * (2.0 * sums[2:3] + ratio * reg_sq)
    image_sq = sums[3:4] + ratio * (2.0 * sums[4:5] + ratio * image_sq)
    step = norm / (image_sq + reg_sq)
    slip[...] = old_slip[...] + step * (field[...] + ratio * way[...])


def to_neighbours(last, first, axis):
    count = lax.axis_size(axis)
    up = [(i, i + 1) for i in range(count - 1)]
    down = [(i + 1, i) for i in range(count - 1)]
    return lax.ppermute(last, axis, up), lax.ppermute(first, axis, down)


def exchanged(pieces, axis):
    return lax.all_to_all(pieces, axis, 0, 0, tiled=True)


def shards(green, data, neighbours, reg_weight):
    row_count, col_count = green.shape
    epochs = data.shape[1]
    n_obs, n_z, n_core = lax.axis_size(OBS), lax.axis_size("z"), lax.axis_size("c")
    n_patch = n_z * n_core
    core = lax.axis_index("c")
    piece = col_count // n_obs
    half = row_count // n_core
    reach = 2 * BAND
    weight_sq = (reg_weight * reg_weight)[None]
    share = row_count // n_patch
    core_scalar = core.astype(jnp.int32)[None]
    place_scalar = lax.axis_index(PATCH).astype(jnp.int32)[None]
    block_scalars = jnp.stack([lax.axis_index(PATCH).astype(jnp.int32), jnp.int32(n_patch)])
    swap = [(0, 1), (1, 0)]
    outward = [(2 * z + 1, 2 * z + 2) for z in range(n_z - 1)]
    outward = outward + [(b, a) for a, b in outward]

    field_shape = ((col_count, epochs), F32)
    image_shape = ((row_count, epochs), F32)
    tail_shape = ((TILE, epochs), F32)
    wide = pltpu.VMEM((row_count, 2 * epochs), BF16)
    near = pltpu.VMEM((col_count + 2 * reach, 2 * epochs), BF16)

    back_matrix = ((col_count, row_count), BF16)
    matrix = ((half, col_count), BF16)
    ids_shape = ((3, BAND), jnp.int32)
    moved, b_high, b_low, own_high, own_low, send = local_call(
        first_back,
        [field_shape, back_matrix, back_matrix, matrix, matrix, ((half, col_count), F32)],
        green, data, scalars=[core_scalar], scratch=[wide], share=share,
    )
    far = lax.ppermute(send, "c", swap)
    pieces = exchanged(moved.reshape(n_obs, piece, epochs), OBS)
    zero_tail = jnp.zeros((TILE, epochs), F32)
    zero_field = jnp.zeros((col_count, epochs), F32)
    spread_shape = ((n_obs, piece + TILE, epochs), F32)
    (out,) = local_call(spread, [spread_shape], pieces, zero_tail)
    every = exchanged(out, OBS)
    edge_shape = ((reach, epochs), F32)
    field, edge, last_ids, first_ids = local_call(
        start_field, [field_shape, edge_shape, ids_shape, ids_shape], every, neighbours,
        scalars=[core_scalar],
    )
    before, after = to_neighbours(last_ids, first_ids, PATCH)
    height, width = col_count + 2 * BAND, col_count + 4 * BAND
    m_matrix = ((col_count, width), BF16)
    m_high, m_low = local_call(
        laplace_square, [m_matrix, m_matrix], before, neighbours, after,
        scalars=[block_scalars],
        scratch=[
            pltpu.VMEM((height, width), BF16),
            pltpu.VMEM((128, 128 + 2 * BAND), BF16),
            pltpu.VMEM((height, TILE), jnp.int32),
        ],
    )
    far_high, far_low = local_call(split_other, [matrix, matrix], far)

    kept, slip, smooth, way = zero_tail, zero_field, zero_field, zero_field
    image = jnp.zeros((row_count, epochs), F32)
    for iteration in range(ITERS):
        other = lax.ppermute(field, "c", swap)
        edge = lax.ppermute(edge, PATCH, outward)
        part, sums, fresh = local_call(
            forward, [((half, epochs), F32), tail_shape, field_shape],
            field, other, edge, weight_sq, smooth,
            own_high, own_low, far_high, far_low, m_high, m_low,
            scalars=[core_scalar],
            scratch=[wide, near],
        )
        pieces = exchanged(part.reshape(n_z, share, epochs), "z")
        if iteration + 1 == ITERS:
            shape = ((n_obs * n_core, TILE, epochs), F32)
            (out,) = local_call(last_sums, [shape], pieces, image, sums, scalars=[place_scalar])
            every = exchanged(out, (*OBS, "c"))
            (out,) = local_call(last_spread, [((n_z, TILE, epochs), F32)], every)
            (slip,) = local_call(
                last_update, [field_shape], exchanged(out, "z"), kept, field, way, slip
            )
            return slip
        (out,) = local_call(collect, [((share + TILE, epochs), F32)], pieces, sums)
        every = lax.all_gather(out, PATCH)
        moved, image, tail, smooth, way, scalars = local_call(
            backward,
            [field_shape, image_shape, tail_shape, field_shape, field_shape, tail_shape],
            every, field, fresh, image, smooth, way, kept, b_high, b_low,
            scratch=[wide],
        )
        pieces = exchanged(moved.reshape(n_obs, piece, epochs), OBS)
        (out,) = local_call(spread, [spread_shape], pieces, tail)
        field, edge, slip, kept = local_call(
            update, [field_shape, edge_shape, field_shape, tail_shape],
            exchanged(out, OBS), scalars, smooth, way, field, slip,
            scalars=[core_scalar],
        )


def solution(mesh):
    split = Mesh(mesh.devices.reshape(4, 4, 16, 2), (*OBS, *PATCH))
    in_specs = (P(OBS, PATCH), P(OBS, None), P(None, PATCH), P())
    return jax.shard_map(
        shards, mesh=split, in_specs=in_specs, out_specs=P(PATCH, None), check_vma=False
    )
```

```python
import functools

import jax
import jax.numpy as jnp
from jax import lax
from jax.experimental import pallas as pl
from jax.experimental.pallas import tpu as pltpu
from jax.sharding import Mesh
from jax.sharding import PartitionSpec as P

BAND = 128
ITERS = 3
OBS = ("x", "y")
PATCH = ("z", "c")
TILE = 8
F32, BF16 = jnp.float32, jnp.bfloat16


def local_call(body, outs, *args, scalars=(), scratch=(), mib=24, **options):
    vmem = pl.BlockSpec(memory_space=pltpu.VMEM)
    smem = pl.BlockSpec(memory_space=pltpu.SMEM)
    return pl.pallas_call(
        functools.partial(body, **options),
        out_shape=[jax.ShapeDtypeStruct(shape, kind) for shape, kind in outs],
        in_specs=[smem] * len(scalars) + [vmem] * len(args),
        out_specs=[vmem] * len(outs),
        scratch_shapes=list(scratch),
        compiler_params=pltpu.CompilerParams(vmem_limit_bytes=mib << 20),
    )(*scalars, *args)


def halves(x):
    high = x.astype(BF16)
    return high, (x - high.astype(F32)).astype(BF16)


def store_halves(ref, start, x):
    high, low = halves(x)
    ref[start : start + x.shape[0], : x.shape[1]] = high
    ref[start : start + x.shape[0], x.shape[1] :] = low


def product(high_ref, low_ref, wide):
    width = wide.shape[1] // 2
    both = jnp.dot(high_ref[...], wide, preferred_element_type=F32)
    both = both + jnp.dot(low_ref[...], wide, preferred_element_type=F32)
    return both[:, :width] + both[:, width:]


def total(x):
    return jnp.sum(x, axis=0, keepdims=True)


def put_rows(ref, rows):
    ref[...] = jnp.zeros_like(ref)
    for place, row in enumerate(rows):
        ref[place : place + 1, :] = row


def summed(pieces_ref):
    value = pieces_ref[0]
    for k in range(1, pieces_ref.shape[0]):
        value = value + pieces_ref[k]
    return value


def first_back(core, place, green, data, moved, back_high, back_low, high, low, send, wide, *, share):
    for k in range(green.shape[0] // 128):
        at = slice(128 * k, 128 * (k + 1))
        back_high[:, at], back_low[:, at] = halves(green[at, :].T)
    store_halves(wide, 0, data[...])
    moved[...] = product(back_high, back_low, wide[...])
    for z in range(0, send.shape[0] // share, 2):
        mine = []
        for k in (z, z + 1):
            start = pl.multiple_of((2 * k + core[0]) * share, TILE)
            mine.append(green[pl.ds(start, share), :])
            start = pl.multiple_of((2 * k + 1 - core[0]) * share, TILE)
            send[share * k : share * (k + 1), :] = green[pl.ds(start, share), :]
        rows = slice(share * z, share * (z + 2))
        high[rows, :], low[rows, :] = halves(jnp.concatenate(mine, 0))


def split_other(other, high, low):
    high[...], low[...] = halves(other[...])


def laplace_square(block, before, ids, after, high, low, rows, own, ids_col, *, n_patch):
    col_count = ids.shape[1]
    height = rows.shape[0]
    total_cols = n_patch * col_count
    start = block[0] * col_count
    relative = jnp.concatenate([before[...], ids[...], after[...]], 1) - (start - 2 * BAND)
    pad = jnp.zeros((TILE - 3, height), jnp.int32)
    ids_col[...] = jnp.concatenate([relative, pad], 0).T
    here = lax.broadcasted_iota(jnp.int32, (1, height), 1) + (start - BAND)
    inside = jnp.where((here >= 0) & (here < total_cols), 1.0, 0.0)
    rows[...] = jnp.zeros_like(rows)
    wide = 128 + 2 * BAND
    for i in range(height // 128):
        at = 128 * i
        row = lax.broadcasted_iota(jnp.int32, (128, wide), 0) + at
        col = lax.broadcasted_iota(jnp.int32, (128, wide), 1) + at
        entry = jnp.where(col == row + BAND, 4.0, 0.0)
        for slot in range(3):
            entry = entry - jnp.where(col == ids_col[at : at + 128, slot : slot + 1], 1.0, 0.0)
        rows[at : at + 128, at : at + wide] = entry.astype(BF16)
    high[...] = jnp.zeros_like(high)
    low[...] = jnp.zeros_like(low)
    for i in range(col_count // 128):
        at = 128 * i
        col = lax.broadcasted_iota(jnp.int32, (128, wide), 0) + at
        row = lax.broadcasted_iota(jnp.int32, (128, wide), 1) + at
        entry = jnp.where(row == col + BAND, 4.0, 0.0)
        for slot in range(3):
            target = relative[slot : slot + 1, at : at + wide]
            entry = entry - jnp.where(col + 2 * BAND == target, 1.0, 0.0)
        own[...] = (entry * inside[:, at : at + wide]).astype(BF16)
        reach = slice(at, at + 128 + 4 * BAND)
        square = jnp.dot(own[...], rows[at : at + wide, reach], preferred_element_type=F32)
        high[at : at + 128, reach], low[at : at + 128, reach] = halves(square)


def forward(core, pair, own_high, own_low, far_high, far_low, part, wide):
    rows = pair.shape[1]
    store_halves(wide, 0, pair[core[0]])
    store_halves(wide, rows, pair[1 - core[0]])
    part[...] = product(own_high, own_low, wide[:rows, :]) + product(far_high, far_low, wide[rows:, :])


def regularized(core, pair, edge, weight, m_high, m_low, near):
    rows, reach = pair.shape[1], 2 * BAND
    own, other = pair[core[0]], pair[1 - core[0]]
    is_first = core[0] == 0
    outer = edge[...]
    store_halves(near, 0, jnp.where(is_first, outer, other[rows - reach :]))
    store_halves(near, reach, own)
    store_halves(near, reach + rows, jnp.where(is_first, other[:reach], outer))
    return own, weight[...] * weight[...] * product(m_high, m_low, near[...])


def gathered(pieces, part):
    part[...] = summed(pieces)


def collect(core, part, pair, edge, weight, smooth, m_high, m_low, out, fresh, near):
    share = part.shape[0]
    out[:share, :] = part[...]
    own, new = regularized(core, pair, edge, weight, m_high, m_low, near)
    fresh[...] = new
    rows = [total(own * own), total(own * new), total(own * smooth[...])]
    out[share:, :] = jnp.concatenate([*rows, jnp.zeros((TILE - 3, own.shape[1]), F32)], 0)


def backward(every, field, fresh, old_image, old_smooth, old_way, old_scalars, high, low, moved, image, tail, smooth, way, scalars, wide):
    count = every.shape[0]
    share = every.shape[1] - TILE
    sums = every[0, share:, :]
    for k in range(1, count):
        sums = sums + every[k, share:, :]
    norm = sums[0:1]
    has_old = old_scalars[2:3, :] > 0.0
    ratio = jnp.where(has_old, norm / old_scalars[0:1, :], 0.0)
    square = jnp.zeros((TILE, every.shape[2]), F32)
    for k in range(0, count, 2):
        rows = slice(share * k, share * (k + 2))
        piece = jnp.concatenate([every[k, :share, :], every[k + 1, :share, :]], 0)
        piece = piece + ratio * old_image[rows, :]
        image[rows, :] = piece
        store_halves(wide, share * k, piece)
        for t in range(2 * share // TILE):
            block = piece[TILE * t : TILE * (t + 1)]
            square = square + block * block
    moved[...] = product(high, low, wide[...])
    put_rows(tail, [total(square)])
    smooth[...] = fresh[...] + ratio * old_smooth[...]
    way[...] = field[...] + ratio * old_way[...]
    reg_sq = sums[1:2] + ratio * (2.0 * sums[2:3] + ratio * old_scalars[1:2, :])
    put_rows(scalars, [norm, reg_sq, jnp.ones_like(norm)])


def spread(pieces, tail, out):
    share = pieces.shape[1]
    value, last = summed(pieces), tail[...]
    for k in range(out.shape[0]):
        out[k, :share, :] = value
        out[k, share:, :] = last


def put_edge(core, field, edge):
    reach = edge.shape[0]
    edge[...] = jnp.where(core[0] == 0, field[:reach, :], field[field.shape[0] - reach :, :])


def start_field(core, every, ids, field, edge, last_ids, first_ids):
    last_ids[...] = ids[:, ids.shape[1] - BAND :]
    first_ids[...] = ids[:, :BAND]
    share = every.shape[1] - TILE
    for k in range(every.shape[0]):
        field[share * k : share * (k + 1), :] = every[k, :share, :]
    put_edge(core, field, edge)


def update(core, every, scalars, smooth, way, old_field, old_slip, field, edge, slip, kept):
    count = every.shape[0]
    share = every.shape[1] - TILE
    image_sq = every[0, share : share + 1, :]
    for k in range(1, count):
        image_sq = image_sq + every[k, share : share + 1, :]
    step = scalars[0:1, :] / (image_sq + scalars[1:2, :])
    for k in range(count):
        rows = slice(share * k, share * (k + 1))
        field[rows, :] = old_field[rows, :] - step * (every[k, :share, :] + smooth[rows, :])
    put_edge(core, field, edge)
    slip[...] = old_slip[...] + step * way[...]
    put_rows(kept, [scalars[0:1, :], scalars[1:2, :], scalars[2:3, :], image_sq])


def last_sums(core, place, share_ref, image, pair, edge, weight, smooth, m_high, m_low, out, near):
    part = share_ref[...]
    share = part.shape[0]
    start = pl.multiple_of(place[0] * share, TILE)
    old = image[pl.ds(start, share), :]
    own, new = regularized(core, pair, edge, weight, m_high, m_low, near)
    rows = [total(own * own), total(own * new), total(own * smooth[...])]
    rows = [*rows, total(part * part), total(part * old)]
    first = jnp.concatenate([*rows, jnp.zeros((TILE - 5, own.shape[1]), F32)], 0)
    for k in range(out.shape[0]):
        out[k] = first


def last_spread(every, out):
    sums, pair = summed(every), every[0] + every[1]
    first = jnp.concatenate([pair[0:3], sums[3:]], 0)
    for k in range(out.shape[0]):
        out[k] = first


def last_update(every, kept, field, way, old_slip, slip):
    sums = summed(every)
    norm, old_norm, reg_sq, image_sq = sums[0:1], kept[0:1, :], kept[1:2, :], kept[3:4, :]
    ratio = norm / old_norm
    reg_sq = sums[1:2] + ratio * (2.0 * sums[2:3] + ratio * reg_sq)
    image_sq = sums[3:4] + ratio * (2.0 * sums[4:5] + ratio * image_sq)
    step = norm / (image_sq + reg_sq)
    slip[...] = old_slip[...] + step * (field[...] + ratio * way[...])


def to_neighbours(last, first, axis):
    count = lax.axis_size(axis)
    up = [(i, i + 1) for i in range(count - 1)]
    down = [(i + 1, i) for i in range(count - 1)]
    return lax.ppermute(last, axis, up), lax.ppermute(first, axis, down)


def exchanged(pieces, axis):
    return lax.all_to_all(pieces, axis, 0, 0, tiled=True)


def shards(green, data, neighbours, reg_weight):
    row_count, col_count = green.shape
    epochs = data.shape[1]
    n_obs, n_z, n_core = lax.axis_size(OBS), lax.axis_size("z"), lax.axis_size("c")
    n_patch = n_z * n_core
    core = lax.axis_index("c")
    piece = col_count // n_obs
    half = row_count // n_core
    reach = 2 * BAND
    weight = reg_weight[None]
    share = row_count // n_patch
    core_scalar = core.astype(jnp.int32)[None]
    place_scalar = lax.axis_index(PATCH).astype(jnp.int32)[None]
    swap = [(0, 1), (1, 0)]
    outward = [(2 * z + 1, 2 * z + 2) for z in range(n_z - 1)]
    outward = outward + [(b, a) for a, b in outward]

    field_shape = ((col_count, epochs), F32)
    image_shape = ((row_count, epochs), F32)
    tail_shape = ((TILE, epochs), F32)
    wide = pltpu.VMEM((row_count, 2 * epochs), BF16)
    near = pltpu.VMEM((col_count + 2 * reach, 2 * epochs), BF16)

    back_matrix = ((col_count, row_count), BF16)
    matrix = ((half, col_count), BF16)
    ids_shape = ((3, BAND), jnp.int32)
    moved, b_high, b_low, own_high, own_low, send = local_call(
        first_back,
        [field_shape, back_matrix, back_matrix, matrix, matrix, ((half, col_count), F32)],
        green, data, scalars=[core_scalar, place_scalar], scratch=[wide], share=share,
    )
    far = lax.ppermute(send, "c", swap)
    pieces = exchanged(moved.reshape(n_obs, piece, epochs), OBS)
    zero_tail = jnp.zeros((TILE, epochs), F32)
    zero_field = jnp.zeros((col_count, epochs), F32)
    spread_shape = ((n_obs, piece + TILE, epochs), F32)
    (out,) = local_call(spread, [spread_shape], pieces, zero_tail)
    every = exchanged(out, OBS)
    edge_shape = ((reach, epochs), F32)
    field, edge, last_ids, first_ids = local_call(
        start_field, [field_shape, edge_shape, ids_shape, ids_shape], every, neighbours,
        scalars=[core_scalar],
    )
    before, after = to_neighbours(last_ids, first_ids, PATCH)
    height, width = col_count + 2 * BAND, col_count + 4 * BAND
    m_matrix = ((col_count, width), BF16)
    m_high, m_low = local_call(
        laplace_square, [m_matrix, m_matrix], before, neighbours, after,
        scalars=[place_scalar],
        n_patch=n_patch,
        scratch=[
            pltpu.VMEM((height, width), BF16),
            pltpu.VMEM((128, 128 + 2 * BAND), BF16),
            pltpu.VMEM((height, TILE), jnp.int32),
        ],
    )
    far_high, far_low = local_call(split_other, [matrix, matrix], far)

    kept, slip, smooth, way = zero_tail, zero_field, zero_field, zero_field
    image = jnp.zeros((row_count, epochs), F32)
    for iteration in range(ITERS):
        edge = lax.ppermute(edge, PATCH, outward)
        pair = lax.all_gather(field, "c")
        (part,) = local_call(
            forward, [((half, epochs), F32)],
            pair, own_high, own_low, far_high, far_low,
            scalars=[core_scalar], scratch=[wide],
        )
        pieces = exchanged(part.reshape(n_z, share, epochs), "z")
        (part,) = local_call(gathered, [((share, epochs), F32)], pieces)
        penalty = (pair, edge, weight, smooth, m_high, m_low)
        if iteration + 1 == ITERS:
            shape = ((n_obs * n_core, TILE, epochs), F32)
            (out,) = local_call(
                last_sums, [shape], part, image, *penalty,
                scalars=[core_scalar, place_scalar], scratch=[near],
            )
            every = exchanged(out, (*OBS, "c"))
            (out,) = local_call(last_spread, [((n_z, TILE, epochs), F32)], every)
            (slip,) = local_call(
                last_update, [field_shape], exchanged(out, "z"), kept, field, way, slip
            )
            return slip
        out, fresh = local_call(
            collect, [((share + TILE, epochs), F32), field_shape], part, *penalty,
            scalars=[core_scalar], scratch=[near],
        )
        every = lax.all_gather(out, PATCH)
        moved, image, tail, smooth, way, scalars = local_call(
            backward,
            [field_shape, image_shape, tail_shape, field_shape, field_shape, tail_shape],
            every, field, fresh, image, smooth, way, kept, b_high, b_low,
            scratch=[wide],
        )
        pieces = exchanged(moved.reshape(n_obs, piece, epochs), OBS)
        (out,) = local_call(spread, [spread_shape], pieces, tail)
        field, edge, slip, kept = local_call(
            update, [field_shape, edge_shape, field_shape, tail_shape],
            exchanged(out, OBS), scalars, smooth, way, field, slip,
            scalars=[core_scalar],
        )


def solution(mesh):
    split = Mesh(mesh.devices.reshape(4, 4, 16, 2), (*OBS, *PATCH))
    in_specs = (P(OBS, PATCH), P(OBS, None), P(None, PATCH), P())

    return jax.shard_map(
        shards, mesh=split, in_specs=in_specs, out_specs=P(PATCH, None), check_vma=False
    )
```

```python
import functools

import jax
import jax.numpy as jnp
from jax import lax
from jax.experimental import pallas as pl
from jax.experimental.pallas import tpu as pltpu
from jax.sharding import Mesh
from jax.sharding import PartitionSpec as P

BAND = 128
ITERS = 3
OBS = ("x", "y")
PATCH = ("z", "c")
TILE = 8
F32, BF16 = jnp.float32, jnp.bfloat16


def local_call(body, outs, *args, scalars=(), scratch=(), mib=24, **options):
    vmem = pl.BlockSpec(memory_space=pltpu.VMEM)
    smem = pl.BlockSpec(memory_space=pltpu.SMEM)
    return pl.pallas_call(
        functools.partial(body, **options),
        out_shape=[jax.ShapeDtypeStruct(shape, kind) for shape, kind in outs],
        in_specs=[smem] * len(scalars) + [vmem] * len(args),
        out_specs=[vmem] * len(outs),
        scratch_shapes=list(scratch),
        compiler_params=pltpu.CompilerParams(vmem_limit_bytes=mib << 20),
    )(*scalars, *args)


def halves(x):
    high = x.astype(BF16)
    return high, (x - high.astype(F32)).astype(BF16)


def store_halves(ref, start, x):
    high, low = halves(x)
    ref[start : start + x.shape[0], : x.shape[1]] = high
    ref[start : start + x.shape[0], x.shape[1] :] = low


def product(high_ref, low_ref, wide):
    width = wide.shape[1] // 2
    both = jnp.dot(high_ref[...], wide, preferred_element_type=F32)
    both = both + jnp.dot(low_ref[...], wide, preferred_element_type=F32)
    return both[:, :width] + both[:, width:]


def total(x):
    return jnp.sum(x, axis=0, keepdims=True)


def put_rows(ref, rows):
    ref[...] = jnp.zeros_like(ref)
    for place, row in enumerate(rows):
        ref[place : place + 1, :] = row


def summed(pieces_ref):
    value = pieces_ref[0]
    for k in range(1, pieces_ref.shape[0]):
        value = value + pieces_ref[k]
    return value


def first_back(core, place, row, green, data, moved, back_high, back_low, high, low, send, wide, *, share):
    for k in range(green.shape[0] // 128):
        at = slice(128 * k, 128 * (k + 1))
        back_high[:, at], back_low[:, at] = halves(green[at, :].T)
    store_halves(wide, 0, data[...])
    moved[...] = product(back_high, back_low, wide[...])
    half = send.shape[0]
    for z in range(0, half // share, 2):
        mine = []
        for k in (z, z + 1):
            start = pl.multiple_of(core[0] * half + k * share, TILE)
            mine.append(green[pl.ds(start, share), :])
            start = pl.multiple_of((1 - core[0]) * half + k * share, TILE)
            send[share * k : share * (k + 1), :] = green[pl.ds(start, share), :]
        rows = slice(share * z, share * (z + 2))
        high[rows, :], low[rows, :] = halves(jnp.concatenate(mine, 0))


def split_other(other, high, low):
    high[...], low[...] = halves(other[...])


def laplace_square(core, block, pair, edge, ids, high, low, rows, own, ids_col, *, n_patch):
    col_count = ids.shape[1]
    height = rows.shape[0]
    total_cols = n_patch * col_count
    start = block[0] * col_count
    own_rows, edge_rows = pair.shape[1] - TILE, edge.shape[0] - TILE
    other = pair[1 - core[0]][own_rows:]
    outer = edge[edge_rows : edge_rows + 3, :]
    is_first = core[0] == 0
    before = jnp.where(is_first, outer, other[3:6]).astype(jnp.int32)
    after = jnp.where(is_first, other[0:3], outer).astype(jnp.int32)
    relative = jnp.concatenate([before, ids[...], after], 1) - (start - 2 * BAND)
    pad = jnp.zeros((TILE - 3, height), jnp.int32)
    ids_col[...] = jnp.concatenate([relative, pad], 0).T
    here = lax.broadcasted_iota(jnp.int32, (1, height), 1) + (start - BAND)
    inside = jnp.where((here >= 0) & (here < total_cols), 1.0, 0.0)
    rows[...] = jnp.zeros_like(rows)
    wide = 128 + 2 * BAND
    for i in range(height // 128):
        at = 128 * i
        row = lax.broadcasted_iota(jnp.int32, (128, wide), 0) + at
        col = lax.broadcasted_iota(jnp.int32, (128, wide), 1) + at
        entry = jnp.where(col == row + BAND, 4.0, 0.0)
        for slot in range(3):
            entry = entry - jnp.where(col == ids_col[at : at + 128, slot : slot + 1], 1.0, 0.0)
        rows[at : at + 128, at : at + wide] = entry.astype(BF16)
    high[...] = jnp.zeros_like(high)
    low[...] = jnp.zeros_like(low)
    for i in range(col_count // 128):
        at = 128 * i
        col = lax.broadcasted_iota(jnp.int32, (128, wide), 0) + at
        row = lax.broadcasted_iota(jnp.int32, (128, wide), 1) + at
        entry = jnp.where(row == col + BAND, 4.0, 0.0)
        for slot in range(3):
            target = relative[slot : slot + 1, at : at + wide]
            entry = entry - jnp.where(col + 2 * BAND == target, 1.0, 0.0)
        own[...] = (entry * inside[:, at : at + wide]).astype(BF16)
        reach = slice(at, at + 128 + 4 * BAND)
        square = jnp.dot(own[...], rows[at : at + wide, reach], preferred_element_type=F32)
        high[at : at + 128, reach], low[at : at + 128, reach] = halves(square)


def forward(core, pair, own_high, own_low, far_high, far_low, part, wide):
    rows = wide.shape[0] // 2
    store_halves(wide, 0, pair[core[0]][:rows])
    store_halves(wide, rows, pair[1 - core[0]][:rows])
    part[...] = product(own_high, own_low, wide[:rows, :]) + product(far_high, far_low, wide[rows:, :])


def regularized(core, pair, edge, weight, m_high, m_low, near):
    reach = 2 * BAND
    rows = near.shape[0] - 2 * reach
    own, other = pair[core[0]][:rows], pair[1 - core[0]][:rows]
    is_first = core[0] == 0
    outer = edge[:reach, :]
    store_halves(near, 0, jnp.where(is_first, outer, other[rows - reach :]))
    store_halves(near, reach, own)
    store_halves(near, reach + rows, jnp.where(is_first, other[:reach], outer))
    return own, weight[...] * weight[...] * product(m_high, m_low, near[...])


def gathered(pieces, part):
    part[...] = summed(pieces)


def collect(core, part, pair, edge, weight, smooth, m_high, m_low, out, fresh, near):
    share = part.shape[0]
    out[:share, :] = part[...]
    own, new = regularized(core, pair, edge, weight, m_high, m_low, near)
    fresh[...] = new
    rows = [total(own * own), total(own * new), total(own * smooth[...])]
    out[share:, :] = jnp.concatenate([*rows, jnp.zeros((TILE - 3, own.shape[1]), F32)], 0)


def backward(every, field, fresh, old_image, old_smooth, old_way, old_scalars, high, low, moved, image, tail, smooth, way, scalars, wide):
    count = every.shape[0]
    share = every.shape[1] - TILE
    sums = every[0, share:, :]
    for k in range(1, count):
        sums = sums + every[k, share:, :]
    norm = sums[0:1]
    has_old = old_scalars[2:3, :] > 0.0
    ratio = jnp.where(has_old, norm / old_scalars[0:1, :], 0.0)
    square = jnp.zeros((TILE, every.shape[2]), F32)
    for k in range(0, count, 2):
        rows = slice(share * k, share * (k + 2))
        piece = jnp.concatenate([every[k, :share, :], every[k + 1, :share, :]], 0)
        piece = piece + ratio * old_image[rows, :]
        image[rows, :] = piece
        store_halves(wide, share * k, piece)
        for t in range(2 * share // TILE):
            block = piece[TILE * t : TILE * (t + 1)]
            square = square + block * block
    moved[...] = product(high, low, wide[...])
    put_rows(tail, [total(square)])
    smooth[...] = fresh[...] + ratio * old_smooth[...]
    way[...] = field[: way.shape[0], :] + ratio * old_way[...]
    reg_sq = sums[1:2] + ratio * (2.0 * sums[2:3] + ratio * old_scalars[1:2, :])
    put_rows(scalars, [norm, reg_sq, jnp.ones_like(norm)])


def spread(pieces, tail, out):
    share = pieces.shape[1]
    value, last = summed(pieces), tail[...]
    for k in range(out.shape[0]):
        out[k, :share, :] = value
        out[k, share:, :] = last


def put_edge(core, rows, field, edge):
    reach = 2 * BAND
    edge[:reach, :] = jnp.where(core[0] == 0, field[:reach, :], field[rows - reach : rows, :])


def start_field(core, every, ids, field, edge):
    share = every.shape[1] - TILE
    rows, reach = field.shape[0] - TILE, edge.shape[0] - TILE
    for k in range(every.shape[0]):
        field[share * k : share * (k + 1), :] = every[k, :share, :]
    put_edge(core, rows, field, edge)
    first, last = ids[:, :BAND].astype(F32), ids[:, ids.shape[1] - BAND :].astype(F32)
    field[rows:, :] = jnp.concatenate([first, last, jnp.zeros((TILE - 6, BAND), F32)], 0)
    sent = jnp.where(core[0] == 0, first, last)
    edge[reach:, :] = jnp.concatenate([sent, jnp.zeros((TILE - 3, BAND), F32)], 0)


def update(core, every, scalars, smooth, way, old_field, old_slip, field, edge, slip, kept):
    count = every.shape[0]
    share = every.shape[1] - TILE
    image_sq = every[0, share : share + 1, :]
    for k in range(1, count):
        image_sq = image_sq + every[k, share : share + 1, :]
    step = scalars[0:1, :] / (image_sq + scalars[1:2, :])
    for k in range(count):
        rows = slice(share * k, share * (k + 1))
        field[rows, :] = old_field[rows, :] - step * (every[k, :share, :] + smooth[rows, :])
    put_edge(core, field.shape[0], field, edge)
    slip[...] = old_slip[...] + step * way[...]
    put_rows(kept, [scalars[0:1, :], scalars[1:2, :], scalars[2:3, :], image_sq])


def last_sums(core, place, share_ref, image, pair, edge, weight, smooth, m_high, m_low, out, near):
    part = share_ref[...]
    share = part.shape[0]
    start = pl.multiple_of(place[0] * share, TILE)
    old = image[pl.ds(start, share), :]
    own, new = regularized(core, pair, edge, weight, m_high, m_low, near)
    rows = [total(own * own), total(own * new), total(own * smooth[...])]
    rows = [*rows, total(part * part), total(part * old)]
    first = jnp.concatenate([*rows, jnp.zeros((TILE - 5, own.shape[1]), F32)], 0)
    for k in range(out.shape[0]):
        out[k] = first


def last_spread(every, out):
    sums, pair = summed(every), every[0] + every[1]
    first = jnp.concatenate([pair[0:3], sums[3:]], 0)
    for k in range(out.shape[0]):
        out[k] = first


def last_update(every, kept, field, way, old_slip, slip):
    sums = summed(every)
    norm, old_norm, reg_sq, image_sq = sums[0:1], kept[0:1, :], kept[1:2, :], kept[3:4, :]
    ratio = norm / old_norm
    reg_sq = sums[1:2] + ratio * (2.0 * sums[2:3] + ratio * reg_sq)
    image_sq = sums[3:4] + ratio * (2.0 * sums[4:5] + ratio * image_sq)
    step = norm / (image_sq + reg_sq)
    slip[...] = old_slip[...] + step * (field[...] + ratio * way[...])


def exchanged(pieces, axis):
    return lax.all_to_all(pieces, axis, 0, 0, tiled=True)


def shards(green, data, neighbours, reg_weight):
    row_count, col_count = green.shape
    epochs = data.shape[1]
    n_obs, n_z, n_core = lax.axis_size(OBS), lax.axis_size("z"), lax.axis_size("c")
    n_patch = n_z * n_core
    core = lax.axis_index("c")
    piece = col_count // n_obs
    half = row_count // n_core
    reach = 2 * BAND
    weight = reg_weight[None]
    share = row_count // n_patch
    core_scalar = core.astype(jnp.int32)[None]
    row_scalar = (core * n_z + lax.axis_index("z")).astype(jnp.int32)[None]
    place_scalar = lax.axis_index(PATCH).astype(jnp.int32)[None]
    swap = [(0, 1), (1, 0)]
    outward = [(2 * z + 1, 2 * z + 2) for z in range(n_z - 1)]
    outward = outward + [(b, a) for a, b in outward]

    field_shape = ((col_count, epochs), F32)
    image_shape = ((row_count, epochs), F32)
    tail_shape = ((TILE, epochs), F32)
    wide = pltpu.VMEM((row_count, 2 * epochs), BF16)
    near = pltpu.VMEM((col_count + 2 * reach, 2 * epochs), BF16)

    back_matrix = ((col_count, row_count), BF16)
    matrix = ((half, col_count), BF16)
    moved, b_high, b_low, own_high, own_low, send = local_call(
        first_back,
        [field_shape, back_matrix, back_matrix, matrix, matrix, ((half, col_count), F32)],
        green, data, scalars=[core_scalar, place_scalar, row_scalar], scratch=[wide], share=share,
    )
    far = lax.ppermute(send, "c", swap)
    pieces = exchanged(moved.reshape(n_obs, piece, epochs), OBS)
    zero_tail = jnp.zeros((TILE, epochs), F32)
    zero_field = jnp.zeros((col_count, epochs), F32)
    spread_shape = ((n_obs, piece + TILE, epochs), F32)
    (out,) = local_call(spread, [spread_shape], pieces, zero_tail)
    every = exchanged(out, OBS)
    edge_shape = ((reach, epochs), F32)
    long_field, long_edge = ((col_count + TILE, epochs), F32), ((reach + TILE, epochs), F32)
    field, edge = local_call(
        start_field, [long_field, long_edge], every, neighbours, scalars=[core_scalar]
    )
    far_high, far_low = local_call(split_other, [matrix, matrix], far)

    kept, slip, smooth, way = zero_tail, zero_field, zero_field, zero_field
    image = jnp.zeros((row_count, epochs), F32)
    for iteration in range(ITERS):
        edge = lax.ppermute(edge, PATCH, outward)
        pair = lax.all_gather(field, "c")
        (part,) = local_call(
            forward, [((half, epochs), F32)],
            pair, own_high, own_low, far_high, far_low,
            scalars=[core_scalar], scratch=[wide],
        )
        pieces = exchanged(part.reshape(n_z, share, epochs), "z")
        (part,) = local_call(gathered, [((share, epochs), F32)], pieces)
        if iteration == 0:
            m_matrix = ((col_count, col_count + 2 * reach), BF16)
            m_high, m_low = local_call(
                laplace_square, [m_matrix, m_matrix], pair, edge, neighbours,
                scalars=[core_scalar, place_scalar],
                n_patch=n_patch,
                scratch=[
                    pltpu.VMEM((col_count + reach, col_count + 2 * reach), BF16),
                    pltpu.VMEM((128, 128 + reach), BF16),
                    pltpu.VMEM((col_count + reach, TILE), jnp.int32),
                ],
            )
        penalty = (pair, edge, weight, smooth, m_high, m_low)
        if iteration + 1 == ITERS:
            shape = ((n_obs * n_core, TILE, epochs), F32)
            (out,) = local_call(
                last_sums, [shape], part, image, *penalty,
                scalars=[core_scalar, row_scalar], scratch=[near],
            )
            every = exchanged(out, (*OBS, "c"))
            (out,) = local_call(last_spread, [((n_z, TILE, epochs), F32)], every)
            (slip,) = local_call(
                last_update, [field_shape], exchanged(out, "z"), kept, field, way, slip
            )
            return slip
        out, fresh = local_call(
            collect, [((share + TILE, epochs), F32), field_shape], part, *penalty,
            scalars=[core_scalar], scratch=[near],
        )
        every = lax.all_gather(lax.all_gather(out, "z"), "c")
        every = every.reshape(n_patch, share + TILE, epochs)
        moved, image, tail, smooth, way, scalars = local_call(
            backward,
            [field_shape, image_shape, tail_shape, field_shape, field_shape, tail_shape],
            every, field, fresh, image, smooth, way, kept, b_high, b_low,
            scratch=[wide],
        )
        pieces = exchanged(moved.reshape(n_obs, piece, epochs), OBS)
        (out,) = local_call(spread, [spread_shape], pieces, tail)
        field, edge, slip, kept = local_call(
            update, [field_shape, edge_shape, field_shape, tail_shape],
            exchanged(out, OBS), scalars, smooth, way, field, slip,
            scalars=[core_scalar],
        )


def solution(mesh):
    split = Mesh(mesh.devices.reshape(4, 4, 16, 2), (*OBS, *PATCH))
    in_specs = (P(OBS, PATCH), P(OBS, None), P(None, PATCH), P())

    return jax.shard_map(
        shards, mesh=split, in_specs=in_specs, out_specs=P(PATCH, None), check_vma=False
    )
```

```python
import functools

import jax
import jax.numpy as jnp
from jax import lax
from jax.experimental import pallas as pl
from jax.experimental.pallas import tpu as pltpu
from jax.sharding import Mesh
from jax.sharding import PartitionSpec as P

BAND = 128
ITERS = 3
OBS = ("x", "y")
PATCH = ("z", "c")
TILE = 8
F32, BF16 = jnp.float32, jnp.bfloat16


def local_call(body, outs, *args, scalars=(), scratch=(), mib=24, **options):
    vmem = pl.BlockSpec(memory_space=pltpu.VMEM)
    smem = pl.BlockSpec(memory_space=pltpu.SMEM)
    return pl.pallas_call(
        functools.partial(body, **options),
        out_shape=[jax.ShapeDtypeStruct(shape, kind) for shape, kind in outs],
        in_specs=[smem] * len(scalars) + [vmem] * len(args),
        out_specs=[vmem] * len(outs),
        scratch_shapes=list(scratch),
        compiler_params=pltpu.CompilerParams(vmem_limit_bytes=mib << 20),
    )(*scalars, *args)


def halves(x):
    high = x.astype(BF16)
    return high, (x - high.astype(F32)).astype(BF16)


def store_halves(ref, start, x):
    high, low = halves(x)
    ref[start : start + x.shape[0], : x.shape[1]] = high
    ref[start : start + x.shape[0], x.shape[1] :] = low


def product(high_ref, low_ref, wide):
    width = wide.shape[1] // 2
    both = jnp.dot(high_ref[...], wide, preferred_element_type=F32)
    both = both + jnp.dot(low_ref[...], wide, preferred_element_type=F32)
    return both[:, :width] + both[:, width:]


def total(x):
    return jnp.sum(x, axis=0, keepdims=True)


def put_rows(ref, rows):
    ref[...] = jnp.zeros_like(ref)
    for place, row in enumerate(rows):
        ref[place : place + 1, :] = row


def summed(pieces_ref):
    value = pieces_ref[0]
    for k in range(1, pieces_ref.shape[0]):
        value = value + pieces_ref[k]
    return value


def first_back(core, place, row, green, data, moved, back_high, back_low, high, low, send, wide, *, share):
    for k in range(green.shape[0] // 128):
        at = slice(128 * k, 128 * (k + 1))
        back_high[:, at], back_low[:, at] = halves(green[at, :].T)
    store_halves(wide, 0, data[...])
    moved[...] = product(back_high, back_low, wide[...])
    half = send.shape[0]
    for z in range(0, half // share, 2):
        mine = []
        for k in (z, z + 1):
            start = pl.multiple_of(core[0] * half + k * share, TILE)
            mine.append(green[pl.ds(start, share), :])
            start = pl.multiple_of((1 - core[0]) * half + k * share, TILE)
            send[share * k : share * (k + 1), :] = green[pl.ds(start, share), :]
        rows = slice(share * z, share * (z + 2))
        high[rows, :], low[rows, :] = halves(jnp.concatenate(mine, 0))


def split_other(other, high, low):
    high[...], low[...] = halves(other[...])


def laplace_square(core, block, pair, edge, ids, high, low, rows, own, ids_col, *, n_patch):
    col_count = ids.shape[1]
    height = rows.shape[0]
    total_cols = n_patch * col_count
    start = block[0] * col_count
    own_rows, edge_rows = pair.shape[1] - TILE, edge.shape[0] - TILE
    other = pair[1 - core[0]][own_rows:]
    outer = edge[edge_rows : edge_rows + 3, :]
    is_first = core[0] == 0
    before = jnp.where(is_first, outer, other[3:6]).astype(jnp.int32)
    after = jnp.where(is_first, other[0:3], outer).astype(jnp.int32)
    relative = jnp.concatenate([before, ids[...], after], 1) - (start - 2 * BAND)
    pad = jnp.zeros((TILE - 3, height), jnp.int32)
    ids_col[...] = jnp.concatenate([relative, pad], 0).T
    here = lax.broadcasted_iota(jnp.int32, (1, height), 1) + (start - BAND)
    inside = jnp.where((here >= 0) & (here < total_cols), 1.0, 0.0)
    rows[...] = jnp.zeros_like(rows)
    wide = 128 + 2 * BAND
    for i in range(height // 128):
        at = 128 * i
        row = lax.broadcasted_iota(jnp.int32, (128, wide), 0) + at
        col = lax.broadcasted_iota(jnp.int32, (128, wide), 1) + at
        entry = jnp.where(col == row + BAND, 4.0, 0.0)
        for slot in range(3):
            entry = entry - jnp.where(col == ids_col[at : at + 128, slot : slot + 1], 1.0, 0.0)
        rows[at : at + 128, at : at + wide] = entry.astype(BF16)
    high[...] = jnp.zeros_like(high)
    low[...] = jnp.zeros_like(low)
    for i in range(col_count // 128):
        at = 128 * i
        col = lax.broadcasted_iota(jnp.int32, (128, wide), 0) + at
        row = lax.broadcasted_iota(jnp.int32, (128, wide), 1) + at
        entry = jnp.where(row == col + BAND, 4.0, 0.0)
        for slot in range(3):
            target = relative[slot : slot + 1, at : at + wide]
            entry = entry - jnp.where(col + 2 * BAND == target, 1.0, 0.0)
        own[...] = (entry * inside[:, at : at + wide]).astype(BF16)
        reach = slice(at, at + 128 + 4 * BAND)
        square = jnp.dot(own[...], rows[at : at + wide, reach], preferred_element_type=F32)
        high[at : at + 128, reach], low[at : at + 128, reach] = halves(square)


def forward(core, pair, own_high, own_low, far_high, far_low, part, wide):
    rows = wide.shape[0] // 2
    store_halves(wide, 0, pair[core[0]][:rows])
    store_halves(wide, rows, pair[1 - core[0]][:rows])
    part[...] = product(own_high, own_low, wide[:rows, :]) + product(far_high, far_low, wide[rows:, :])


def regularized(core, pair, edge, weight, m_high, m_low, near):
    reach = 2 * BAND
    rows = near.shape[0] - 2 * reach
    own, other = pair[core[0]][:rows], pair[1 - core[0]][:rows]
    is_first = core[0] == 0
    outer = edge[:reach, :]
    store_halves(near, 0, jnp.where(is_first, outer, other[rows - reach :]))
    store_halves(near, reach, own)
    store_halves(near, reach + rows, jnp.where(is_first, other[:reach], outer))
    return own, weight[...] * weight[...] * product(m_high, m_low, near[...])


def gathered(pieces, part):
    part[...] = summed(pieces)


def collect(core, part, pair, edge, weight, smooth, m_high, m_low, out, fresh, near):
    share = part.shape[0]
    own, new = regularized(core, pair, edge, weight, m_high, m_low, near)
    fresh[...] = new
    rows = [total(own * own), total(own * new), total(own * smooth[...])]
    value, tail = part[...], jnp.concatenate([*rows, jnp.zeros((TILE - 3, own.shape[1]), F32)], 0)
    for k in range(out.shape[0]):
        out[k, :share, :] = value
        out[k, share:, :] = tail


def backward(every, field, fresh, old_image, old_smooth, old_way, old_scalars, high, low, moved, image, tail, smooth, way, scalars, wide):
    count = every.shape[0]
    share = every.shape[1] - TILE
    sums = every[0, share:, :]
    for k in range(1, count):
        sums = sums + every[k, share:, :]
    norm = sums[0:1]
    has_old = old_scalars[2:3, :] > 0.0
    ratio = jnp.where(has_old, norm / old_scalars[0:1, :], 0.0)
    square = jnp.zeros((TILE, every.shape[2]), F32)
    for k in range(0, count, 2):
        rows = slice(share * k, share * (k + 2))
        piece = jnp.concatenate([every[k, :share, :], every[k + 1, :share, :]], 0)
        piece = piece + ratio * old_image[rows, :]
        image[rows, :] = piece
        store_halves(wide, share * k, piece)
        for t in range(2 * share // TILE):
            block = piece[TILE * t : TILE * (t + 1)]
            square = square + block * block
    moved[...] = product(high, low, wide[...])
    put_rows(tail, [total(square)])
    smooth[...] = fresh[...] + ratio * old_smooth[...]
    way[...] = field[: way.shape[0], :] + ratio * old_way[...]
    reg_sq = sums[1:2] + ratio * (2.0 * sums[2:3] + ratio * old_scalars[1:2, :])
    put_rows(scalars, [norm, reg_sq, jnp.ones_like(norm)])


def spread(pieces, tail, out):
    share = pieces.shape[1]
    value, last = summed(pieces), tail[...]
    for k in range(out.shape[0]):
        out[k, :share, :] = value
        out[k, share:, :] = last


def put_edge(core, rows, field, edge):
    reach = 2 * BAND
    edge[:reach, :] = jnp.where(core[0] == 0, field[:reach, :], field[rows - reach : rows, :])


def start_field(core, every, ids, field, edge):
    share = every.shape[1] - TILE
    rows, reach = field.shape[0] - TILE, edge.shape[0] - TILE
    for k in range(every.shape[0]):
        field[share * k : share * (k + 1), :] = every[k, :share, :]
    put_edge(core, rows, field, edge)
    first, last = ids[:, :BAND].astype(F32), ids[:, ids.shape[1] - BAND :].astype(F32)
    field[rows:, :] = jnp.concatenate([first, last, jnp.zeros((TILE - 6, BAND), F32)], 0)
    sent = jnp.where(core[0] == 0, first, last)
    edge[reach:, :] = jnp.concatenate([sent, jnp.zeros((TILE - 3, BAND), F32)], 0)


def update(core, every, scalars, smooth, way, old_field, old_slip, field, edge, slip, kept):
    count = every.shape[0]
    share = every.shape[1] - TILE
    image_sq = every[0, share : share + 1, :]
    for k in range(1, count):
        image_sq = image_sq + every[k, share : share + 1, :]
    step = scalars[0:1, :] / (image_sq + scalars[1:2, :])
    for k in range(count):
        rows = slice(share * k, share * (k + 1))
        field[rows, :] = old_field[rows, :] - step * (every[k, :share, :] + smooth[rows, :])
    put_edge(core, field.shape[0], field, edge)
    slip[...] = old_slip[...] + step * way[...]
    put_rows(kept, [scalars[0:1, :], scalars[1:2, :], scalars[2:3, :], image_sq])


def last_sums(core, place, share_ref, image, pair, edge, weight, smooth, m_high, m_low, out, near):
    part = share_ref[...]
    share = part.shape[0]
    start = pl.multiple_of(place[0] * share, TILE)
    old = image[pl.ds(start, share), :]
    own, new = regularized(core, pair, edge, weight, m_high, m_low, near)
    rows = [total(own * own), total(own * new), total(own * smooth[...])]
    rows = [*rows, total(part * part), total(part * old)]
    first = jnp.concatenate([*rows, jnp.zeros((TILE - 5, own.shape[1]), F32)], 0)
    for k in range(out.shape[0]):
        out[k] = first


def last_spread(every, out):
    sums, pair = summed(every), every[0] + every[1]
    first = jnp.concatenate([pair[0:3], sums[3:]], 0)
    for k in range(out.shape[0]):
        out[k] = first


def last_update(every, kept, field, way, old_slip, slip):
    sums = summed(every)
    norm, old_norm, reg_sq, image_sq = sums[0:1], kept[0:1, :], kept[1:2, :], kept[3:4, :]
    ratio = norm / old_norm
    reg_sq = sums[1:2] + ratio * (2.0 * sums[2:3] + ratio * reg_sq)
    image_sq = sums[3:4] + ratio * (2.0 * sums[4:5] + ratio * image_sq)
    step = norm / (image_sq + reg_sq)
    slip[...] = old_slip[...] + step * (field[...] + ratio * way[...])


def exchanged(pieces, axis):
    return lax.all_to_all(pieces, axis, 0, 0, tiled=True)


def shards(green, data, neighbours, reg_weight):
    row_count, col_count = green.shape
    epochs = data.shape[1]
    n_obs, n_z, n_core = lax.axis_size(OBS), lax.axis_size("z"), lax.axis_size("c")
    n_patch = n_z * n_core
    core = lax.axis_index("c")
    piece = col_count // n_obs
    half = row_count // n_core
    reach = 2 * BAND
    weight = reg_weight[None]
    share = row_count // n_patch
    core_scalar = core.astype(jnp.int32)[None]
    row_scalar = (core * n_z + lax.axis_index("z")).astype(jnp.int32)[None]
    place_scalar = lax.axis_index(PATCH).astype(jnp.int32)[None]
    swap = [(0, 1), (1, 0)]
    outward = [(2 * z + 1, 2 * z + 2) for z in range(n_z - 1)]
    outward = outward + [(b, a) for a, b in outward]

    field_shape = ((col_count, epochs), F32)
    image_shape = ((row_count, epochs), F32)
    tail_shape = ((TILE, epochs), F32)
    wide = pltpu.VMEM((row_count, 2 * epochs), BF16)
    near = pltpu.VMEM((col_count + 2 * reach, 2 * epochs), BF16)

    back_matrix = ((col_count, row_count), BF16)
    matrix = ((half, col_count), BF16)
    moved, b_high, b_low, own_high, own_low, send = local_call(
        first_back,
        [field_shape, back_matrix, back_matrix, matrix, matrix, ((half, col_count), F32)],
        green, data, scalars=[core_scalar, place_scalar, row_scalar], scratch=[wide], share=share,
    )
    far = lax.ppermute(send, "c", swap)
    pieces = exchanged(moved.reshape(n_obs, piece, epochs), OBS)
    zero_tail = jnp.zeros((TILE, epochs), F32)
    zero_field = jnp.zeros((col_count, epochs), F32)
    spread_shape = ((n_obs, piece + TILE, epochs), F32)
    (out,) = local_call(spread, [spread_shape], pieces, zero_tail)
    every = exchanged(out, OBS)
    edge_shape = ((reach, epochs), F32)
    long_field, long_edge = ((col_count + TILE, epochs), F32), ((reach + TILE, epochs), F32)
    field, edge = local_call(
        start_field, [long_field, long_edge], every, neighbours, scalars=[core_scalar]
    )
    far_high, far_low = local_call(split_other, [matrix, matrix], far)

    kept, slip, smooth, way = zero_tail, zero_field, zero_field, zero_field
    image = jnp.zeros((row_count, epochs), F32)
    for iteration in range(ITERS):
        edge = lax.ppermute(edge, PATCH, outward)
        pair = lax.all_gather(field, "c")
        (part,) = local_call(
            forward, [((half, epochs), F32)],
            pair, own_high, own_low, far_high, far_low,
            scalars=[core_scalar], scratch=[wide],
        )
        pieces = exchanged(part.reshape(n_z, share, epochs), "z")
        (part,) = local_call(gathered, [((share, epochs), F32)], pieces)
        if iteration == 0:
            m_matrix = ((col_count, col_count + 2 * reach), BF16)
            m_high, m_low = local_call(
                laplace_square, [m_matrix, m_matrix], pair, edge, neighbours,
                scalars=[core_scalar, place_scalar],
                n_patch=n_patch,
                scratch=[
                    pltpu.VMEM((col_count + reach, col_count + 2 * reach), BF16),
                    pltpu.VMEM((128, 128 + reach), BF16),
                    pltpu.VMEM((col_count + reach, TILE), jnp.int32),
                ],
            )
        penalty = (pair, edge, weight, smooth, m_high, m_low)
        if iteration + 1 == ITERS:
            shape = ((n_obs * n_core, TILE, epochs), F32)
            (out,) = local_call(
                last_sums, [shape], part, image, *penalty,
                scalars=[core_scalar, row_scalar], scratch=[near],
            )
            every = exchanged(out, (*OBS, "c"))
            (out,) = local_call(last_spread, [((n_z, TILE, epochs), F32)], every)
            (slip,) = local_call(
                last_update, [field_shape], exchanged(out, "z"), kept, field, way, slip
            )
            return slip
        out, fresh = local_call(
            collect, [((n_z, share + TILE, epochs), F32), field_shape], part, *penalty,
            scalars=[core_scalar], scratch=[near],
        )
        every = lax.all_gather(exchanged(out, "z"), "c")
        every = every.reshape(n_patch, share + TILE, epochs)
        moved, image, tail, smooth, way, scalars = local_call(
            backward,
            [field_shape, image_shape, tail_shape, field_shape, field_shape, tail_shape],
            every, field, fresh, image, smooth, way, kept, b_high, b_low,
            scratch=[wide],
        )
        pieces = exchanged(moved.reshape(n_obs, piece, epochs), OBS)
        (out,) = local_call(spread, [spread_shape], pieces, tail)
        field, edge, slip, kept = local_call(
            update, [field_shape, edge_shape, field_shape, tail_shape],
            exchanged(out, OBS), scalars, smooth, way, field, slip,
            scalars=[core_scalar],
        )


def solution(mesh):
    split = Mesh(mesh.devices.reshape(4, 4, 16, 2), (*OBS, *PATCH))
    in_specs = (P(OBS, PATCH), P(OBS, None), P(None, PATCH), P())

    return jax.shard_map(
        shards, mesh=split, in_specs=in_specs, out_specs=P(PATCH, None), check_vma=False
    )
```

```python
import functools

import jax
import jax.numpy as jnp
from jax import lax
from jax.experimental import pallas as pl
from jax.experimental.pallas import tpu as pltpu
from jax.sharding import Mesh
from jax.sharding import PartitionSpec as P

BAND = 128
ITERS = 3
OBS = ("x", "y")
Z = ("zh", "zl")
PATCH = (*Z, "c")
TILE = 8
F32, BF16 = jnp.float32, jnp.bfloat16


def local_call(body, outs, *args, scalars=(), scratch=(), mib=24, **options):
    vmem = pl.BlockSpec(memory_space=pltpu.VMEM)
    smem = pl.BlockSpec(memory_space=pltpu.SMEM)
    return pl.pallas_call(
        functools.partial(body, **options),
        out_shape=[jax.ShapeDtypeStruct(shape, kind) for shape, kind in outs],
        in_specs=[smem] * len(scalars) + [vmem] * len(args),
        out_specs=[vmem] * len(outs),
        scratch_shapes=list(scratch),
        compiler_params=pltpu.CompilerParams(vmem_limit_bytes=mib << 20),
    )(*scalars, *args)


def halves(x):
    high = x.astype(BF16)
    return high, (x - high.astype(F32)).astype(BF16)


def store_halves(ref, start, x):
    high, low = halves(x)
    ref[start : start + x.shape[0], : x.shape[1]] = high
    ref[start : start + x.shape[0], x.shape[1] :] = low


def product(high_ref, low_ref, wide):
    width = wide.shape[1] // 2
    both = jnp.dot(high_ref[...], wide, preferred_element_type=F32)
    both = both + jnp.dot(low_ref[...], wide, preferred_element_type=F32)
    return both[:, :width] + both[:, width:]


def total(x):
    return jnp.sum(x, axis=0, keepdims=True)


def put_rows(ref, rows):
    ref[...] = jnp.zeros_like(ref)
    for place, row in enumerate(rows):
        ref[place : place + 1, :] = row


def summed(pieces_ref):
    value = pieces_ref[0]
    for k in range(1, pieces_ref.shape[0]):
        value = value + pieces_ref[k]
    return value


def first_back(core, place, row, green, data, moved, back_high, back_low, high, low, send, wide, *, share):
    for k in range(green.shape[0] // 128):
        at = slice(128 * k, 128 * (k + 1))
        back_high[:, at], back_low[:, at] = halves(green[at, :].T)
    store_halves(wide, 0, data[...])
    moved[...] = product(back_high, back_low, wide[...])
    half = send.shape[0]
    for z in range(0, half // share, 2):
        mine = []
        for k in (z, z + 1):
            start = pl.multiple_of((4 * (k // 2) + 2 * core[0] + k % 2) * share, TILE)
            mine.append(green[pl.ds(start, share), :])
            start = pl.multiple_of((4 * (k // 2) + 2 * (1 - core[0]) + k % 2) * share, TILE)
            send[share * k : share * (k + 1), :] = green[pl.ds(start, share), :]
        rows = slice(share * z, share * (z + 2))
        high[rows, :], low[rows, :] = halves(jnp.concatenate(mine, 0))


def split_other(other, high, low):
    high[...], low[...] = halves(other[...])


def laplace_square(core, block, pair, edge, ids, high, low, rows, own, ids_col, *, n_patch):
    col_count = ids.shape[1]
    height = rows.shape[0]
    total_cols = n_patch * col_count
    start = block[0] * col_count
    own_rows, edge_rows = pair.shape[1] - TILE, edge.shape[0] - TILE
    other = pair[1 - core[0]][own_rows:]
    outer = edge[edge_rows : edge_rows + 3, :]
    is_first = core[0] == 0
    before = jnp.where(is_first, outer, other[3:6]).astype(jnp.int32)
    after = jnp.where(is_first, other[0:3], outer).astype(jnp.int32)
    relative = jnp.concatenate([before, ids[...], after], 1) - (start - 2 * BAND)
    pad = jnp.zeros((TILE - 3, height), jnp.int32)
    ids_col[...] = jnp.concatenate([relative, pad], 0).T
    here = lax.broadcasted_iota(jnp.int32, (1, height), 1) + (start - BAND)
    inside = jnp.where((here >= 0) & (here < total_cols), 1.0, 0.0)
    rows[...] = jnp.zeros_like(rows)
    wide = 128 + 2 * BAND
    for i in range(height // 128):
        at = 128 * i
        row = lax.broadcasted_iota(jnp.int32, (128, wide), 0) + at
        col = lax.broadcasted_iota(jnp.int32, (128, wide), 1) + at
        entry = jnp.where(col == row + BAND, 4.0, 0.0)
        for slot in range(3):
            entry = entry - jnp.where(col == ids_col[at : at + 128, slot : slot + 1], 1.0, 0.0)
        rows[at : at + 128, at : at + wide] = entry.astype(BF16)
    high[...] = jnp.zeros_like(high)
    low[...] = jnp.zeros_like(low)
    for i in range(col_count // 128):
        at = 128 * i
        col = lax.broadcasted_iota(jnp.int32, (128, wide), 0) + at
        row = lax.broadcasted_iota(jnp.int32, (128, wide), 1) + at
        entry = jnp.where(row == col + BAND, 4.0, 0.0)
        for slot in range(3):
            target = relative[slot : slot + 1, at : at + wide]
            entry = entry - jnp.where(col + 2 * BAND == target, 1.0, 0.0)
        own[...] = (entry * inside[:, at : at + wide]).astype(BF16)
        reach = slice(at, at + 128 + 4 * BAND)
        square = jnp.dot(own[...], rows[at : at + wide, reach], preferred_element_type=F32)
        high[at : at + 128, reach], low[at : at + 128, reach] = halves(square)


def forward(core, pair, own_high, own_low, far_high, far_low, part, wide):
    rows = wide.shape[0] // 2
    store_halves(wide, 0, pair[core[0]][:rows])
    store_halves(wide, rows, pair[1 - core[0]][:rows])
    part[...] = product(own_high, own_low, wide[:rows, :]) + product(far_high, far_low, wide[rows:, :])


def regularized(core, pair, edge, weight, m_high, m_low, near):
    reach = 2 * BAND
    rows = near.shape[0] - 2 * reach
    own, other = pair[core[0]][:rows], pair[1 - core[0]][:rows]
    is_first = core[0] == 0
    outer = edge[:reach, :]
    store_halves(near, 0, jnp.where(is_first, outer, other[rows - reach :]))
    store_halves(near, reach, own)
    store_halves(near, reach + rows, jnp.where(is_first, other[:reach], outer))
    return own, weight[...] * weight[...] * product(m_high, m_low, near[...])


def gathered(pieces, part):
    part[...] = summed(pieces)


def collect(core, part, pair, edge, weight, smooth, m_high, m_low, out, fresh, near):
    share = part.shape[0]
    out[:share, :] = part[...]
    own, new = regularized(core, pair, edge, weight, m_high, m_low, near)
    fresh[...] = new
    rows = [total(own * own), total(own * new), total(own * smooth[...])]
    out[share:, :] = jnp.concatenate([*rows, jnp.zeros((TILE - 3, own.shape[1]), F32)], 0)


def backward(every, field, fresh, old_image, old_smooth, old_way, old_scalars, high, low, moved, image, tail, smooth, way, scalars, wide):
    count = every.shape[0]
    share = every.shape[1] - TILE
    sums = every[0, share:, :]
    for k in range(1, count):
        sums = sums + every[k, share:, :]
    norm = sums[0:1]
    has_old = old_scalars[2:3, :] > 0.0
    ratio = jnp.where(has_old, norm / old_scalars[0:1, :], 0.0)
    square = jnp.zeros((TILE, every.shape[2]), F32)
    for k in range(0, count, 2):
        rows = slice(share * k, share * (k + 2))
        piece = jnp.concatenate([every[k, :share, :], every[k + 1, :share, :]], 0)
        piece = piece + ratio * old_image[rows, :]
        image[rows, :] = piece
        store_halves(wide, share * k, piece)
        for t in range(2 * share // TILE):
            block = piece[TILE * t : TILE * (t + 1)]
            square = square + block * block
    moved[...] = product(high, low, wide[...])
    put_rows(tail, [total(square)])
    smooth[...] = fresh[...] + ratio * old_smooth[...]
    way[...] = field[: way.shape[0], :] + ratio * old_way[...]
    reg_sq = sums[1:2] + ratio * (2.0 * sums[2:3] + ratio * old_scalars[1:2, :])
    put_rows(scalars, [norm, reg_sq, jnp.ones_like(norm)])


def spread(pieces, tail, out):
    share = pieces.shape[1]
    value, last = summed(pieces), tail[...]
    for k in range(out.shape[0]):
        out[k, :share, :] = value
        out[k, share:, :] = last


def spread_first(pieces, out):
    value = summed(pieces)
    for k in range(out.shape[0]):
        out[k] = value


def put_edge(core, rows, field, edge):
    reach = 2 * BAND
    edge[:reach, :] = jnp.where(core[0] == 0, field[:reach, :], field[rows - reach : rows, :])


def start_field(core, every, ids, field, edge):
    share = every.shape[1]
    rows, reach = field.shape[0] - TILE, edge.shape[0] - TILE
    for k in range(every.shape[0]):
        field[share * k : share * (k + 1), :] = every[k]
    put_edge(core, rows, field, edge)
    first, last = ids[:, :BAND].astype(F32), ids[:, ids.shape[1] - BAND :].astype(F32)
    field[rows:, :] = jnp.concatenate([first, last, jnp.zeros((TILE - 6, BAND), F32)], 0)
    sent = jnp.where(core[0] == 0, first, last)
    edge[reach:, :] = jnp.concatenate([sent, jnp.zeros((TILE - 3, BAND), F32)], 0)


def update(core, every, scalars, smooth, way, old_field, old_slip, field, edge, slip, kept):
    count = every.shape[0]
    share = every.shape[1] - TILE
    image_sq = every[0, share : share + 1, :]
    for k in range(1, count):
        image_sq = image_sq + every[k, share : share + 1, :]
    step = scalars[0:1, :] / (image_sq + scalars[1:2, :])
    for k in range(count):
        rows = slice(share * k, share * (k + 1))
        field[rows, :] = old_field[rows, :] - step * (every[k, :share, :] + smooth[rows, :])
    put_edge(core, field.shape[0], field, edge)
    slip[...] = old_slip[...] + step * way[...]
    put_rows(kept, [scalars[0:1, :], scalars[1:2, :], scalars[2:3, :], image_sq])


def last_sums(core, place, share_ref, image, pair, edge, weight, smooth, m_high, m_low, out, near):
    part = share_ref[...]
    share = part.shape[0]
    start = pl.multiple_of(place[0] * share, TILE)
    old = image[pl.ds(start, share), :]
    own, new = regularized(core, pair, edge, weight, m_high, m_low, near)
    rows = [total(own * own), total(own * new), total(own * smooth[...])]
    rows = [*rows, total(part * part), total(part * old)]
    first = jnp.concatenate([*rows, jnp.zeros((TILE - 5, own.shape[1]), F32)], 0)
    for k in range(out.shape[0]):
        out[k] = first


def last_spread(every, out):
    sums, pair = summed(every), every[0] + every[1]
    first = jnp.concatenate([pair[0:3], sums[3:]], 0)
    for k in range(out.shape[0]):
        out[k] = first


def last_update(every, kept, field, way, old_slip, slip):
    sums = summed(every)
    norm, old_norm, reg_sq, image_sq = sums[0:1], kept[0:1, :], kept[1:2, :], kept[3:4, :]
    ratio = norm / old_norm
    reg_sq = sums[1:2] + ratio * (2.0 * sums[2:3] + ratio * reg_sq)
    image_sq = sums[3:4] + ratio * (2.0 * sums[4:5] + ratio * image_sq)
    step = norm / (image_sq + reg_sq)
    slip[...] = old_slip[...] + step * (field[...] + ratio * way[...])


def exchanged(pieces, axis):
    return lax.all_to_all(pieces, axis, 0, 0, tiled=True)


def shards(green, data, neighbours, reg_weight):
    row_count, col_count = green.shape
    epochs = data.shape[1]
    n_obs, n_z, n_core = lax.axis_size(OBS), lax.axis_size(Z), lax.axis_size("c")
    n_patch = n_z * n_core
    core = lax.axis_index("c")
    piece = col_count // n_obs
    half = row_count // n_core
    reach = 2 * BAND
    weight = reg_weight[None]
    share = row_count // n_patch
    core_scalar = core.astype(jnp.int32)[None]
    row_scalar = lax.axis_index(("zh", "c", "zl")).astype(jnp.int32)[None]
    place_scalar = lax.axis_index(PATCH).astype(jnp.int32)[None]
    swap = [(0, 1), (1, 0)]
    outward = [(2 * z + 1, 2 * z + 2) for z in range(n_z - 1)]
    outward = outward + [(b, a) for a, b in outward]

    field_shape = ((col_count, epochs), F32)
    image_shape = ((row_count, epochs), F32)
    tail_shape = ((TILE, epochs), F32)
    wide = pltpu.VMEM((row_count, 2 * epochs), BF16)
    near = pltpu.VMEM((col_count + 2 * reach, 2 * epochs), BF16)

    back_matrix = ((col_count, row_count), BF16)
    matrix = ((half, col_count), BF16)
    moved, b_high, b_low, own_high, own_low, send = local_call(
        first_back,
        [field_shape, back_matrix, back_matrix, matrix, matrix, ((half, col_count), F32)],
        green, data, scalars=[core_scalar, place_scalar, row_scalar], scratch=[wide], share=share,
    )
    far = lax.ppermute(send, "c", swap)
    pieces = exchanged(moved.reshape(n_obs, piece, epochs), OBS)
    zero_tail = jnp.zeros((TILE, epochs), F32)
    zero_field = jnp.zeros((col_count, epochs), F32)
    spread_shape = ((n_obs, piece + TILE, epochs), F32)
    (out,) = local_call(spread_first, [((n_obs, piece, epochs), F32)], pieces)
    every = exchanged(out, OBS)
    edge_shape = ((reach, epochs), F32)
    long_field, long_edge = ((col_count + TILE, epochs), F32), ((reach + TILE, epochs), F32)
    field, edge = local_call(
        start_field, [long_field, long_edge], every, neighbours, scalars=[core_scalar]
    )
    far_high, far_low = local_call(split_other, [matrix, matrix], far)

    kept, slip, smooth, way = zero_tail, zero_field, zero_field, zero_field
    image = jnp.zeros((row_count, epochs), F32)
    for iteration in range(ITERS):
        edge = lax.ppermute(edge, PATCH, outward)
        pair = lax.all_gather(field, "c")
        (part,) = local_call(
            forward, [((half, epochs), F32)],
            pair, own_high, own_low, far_high, far_low,
            scalars=[core_scalar], scratch=[wide],
        )
        pieces = exchanged(part.reshape(n_z, share, epochs), Z)
        (part,) = local_call(gathered, [((share, epochs), F32)], pieces)
        if iteration == 0:
            m_matrix = ((col_count, col_count + 2 * reach), BF16)
            m_high, m_low = local_call(
                laplace_square, [m_matrix, m_matrix], pair, edge, neighbours,
                scalars=[core_scalar, place_scalar],
                n_patch=n_patch,
                scratch=[
                    pltpu.VMEM((col_count + reach, col_count + 2 * reach), BF16),
                    pltpu.VMEM((128, 128 + reach), BF16),
                    pltpu.VMEM((col_count + reach, TILE), jnp.int32),
                ],
            )
        penalty = (pair, edge, weight, smooth, m_high, m_low)
        if iteration + 1 == ITERS:
            shape = ((n_obs * n_core, TILE, epochs), F32)
            (out,) = local_call(
                last_sums, [shape], part, image, *penalty,
                scalars=[core_scalar, row_scalar], scratch=[near],
            )
            every = exchanged(out, (*OBS, "c"))
            (out,) = local_call(last_spread, [((n_z, TILE, epochs), F32)], every)
            (slip,) = local_call(
                last_update, [field_shape], exchanged(out, Z), kept, field, way, slip
            )
            return slip
        out, fresh = local_call(
            collect, [((share + TILE, epochs), F32), field_shape], part, *penalty,
            scalars=[core_scalar], scratch=[near],
        )
        every = lax.all_gather(lax.all_gather(out, "zl"), ("zh", "c"))
        every = every.reshape(n_patch, share + TILE, epochs)
        moved, image, tail, smooth, way, scalars = local_call(
            backward,
            [field_shape, image_shape, tail_shape, field_shape, field_shape, tail_shape],
            every, field, fresh, image, smooth, way, kept, b_high, b_low,
            scratch=[wide],
        )
        pieces = exchanged(moved.reshape(n_obs, piece, epochs), OBS)
        (out,) = local_call(spread, [spread_shape], pieces, tail)
        field, edge, slip, kept = local_call(
            update, [field_shape, edge_shape, field_shape, tail_shape],
            exchanged(out, OBS), scalars, smooth, way, field, slip,
            scalars=[core_scalar],
        )


def solution(mesh):
    split = Mesh(mesh.devices.reshape(4, 4, 8, 2, 2), (*OBS, *PATCH))
    in_specs = (P(OBS, PATCH), P(OBS, None), P(None, PATCH), P())

    return jax.shard_map(
        shards, mesh=split, in_specs=in_specs, out_specs=P(PATCH, None), check_vma=False
    )
```

```python
import functools

import jax
import jax.numpy as jnp
from jax import lax
from jax.experimental import pallas as pl
from jax.experimental.pallas import tpu as pltpu
from jax.sharding import Mesh
from jax.sharding import PartitionSpec as P

BAND = 128
ITERS = 3
OBS = ("x", "y")
Z = ("zh", "zl")
PATCH = (*Z, "c")
TILE = 8
F32, BF16 = jnp.float32, jnp.bfloat16


def local_call(body, outs, *args, scalars=(), scratch=(), mib=24, **options):
    vmem = pl.BlockSpec(memory_space=pltpu.VMEM)
    smem = pl.BlockSpec(memory_space=pltpu.SMEM)
    return pl.pallas_call(
        functools.partial(body, **options),
        out_shape=[jax.ShapeDtypeStruct(shape, kind) for shape, kind in outs],
        in_specs=[smem] * len(scalars) + [vmem] * len(args),
        out_specs=[vmem] * len(outs),
        scratch_shapes=list(scratch),
        compiler_params=pltpu.CompilerParams(vmem_limit_bytes=mib << 20),
    )(*scalars, *args)


def halves(x):
    high = x.astype(BF16)
    return high, (x - high.astype(F32)).astype(BF16)


def store_halves(ref, start, x):
    high, low = halves(x)
    ref[start : start + x.shape[0], : x.shape[1]] = high
    ref[start : start + x.shape[0], x.shape[1] :] = low


def product(high_ref, low_ref, wide):
    width = wide.shape[1] // 2
    both = jnp.dot(high_ref[...], wide, preferred_element_type=F32)
    both = both + jnp.dot(low_ref[...], wide, preferred_element_type=F32)
    return both[:, :width] + both[:, width:]


def total(x):
    return jnp.sum(x, axis=0, keepdims=True)


def put_rows(ref, rows):
    ref[...] = jnp.zeros_like(ref)
    for place, row in enumerate(rows):
        ref[place : place + 1, :] = row


def summed(pieces_ref):
    value = pieces_ref[0]
    for k in range(1, pieces_ref.shape[0]):
        value = value + pieces_ref[k]
    return value


def first_back(core, place, row, green, data, moved, back_high, back_low, high, low, send, wide, *, share):
    for k in range(green.shape[0] // 128):
        at = slice(128 * k, 128 * (k + 1))
        back_high[:, at], back_low[:, at] = halves(green[at, :].T)
    store_halves(wide, 0, data[...])
    moved[...] = product(back_high, back_low, wide[...])
    half = send.shape[0]
    far_count = half // (2 * share)
    for z in range(0, half // share, 2):
        mine = []
        for k in (z, z + 1):
            start = pl.multiple_of((4 * (k % far_count) + 2 * core[0] + k // far_count) * share, TILE)
            mine.append(green[pl.ds(start, share), :])
            start = pl.multiple_of((4 * (k % far_count) + 2 * (1 - core[0]) + k // far_count) * share, TILE)
            send[share * k : share * (k + 1), :] = green[pl.ds(start, share), :]
        rows = slice(share * z, share * (z + 2))
        high[rows, :], low[rows, :] = halves(jnp.concatenate(mine, 0))


def split_other(other, high, low):
    high[...], low[...] = halves(other[...])


def laplace_square(core, block, pair, edge, ids, high, low, rows, own, ids_col, *, n_patch):
    col_count = ids.shape[1]
    height = rows.shape[0]
    total_cols = n_patch * col_count
    start = block[0] * col_count
    own_rows, edge_rows = pair.shape[1] - TILE, edge.shape[0] - TILE
    other = pair[1 - core[0]][own_rows:]
    outer = edge[edge_rows : edge_rows + 3, :]
    is_first = core[0] == 0
    before = jnp.where(is_first, outer, other[3:6]).astype(jnp.int32)
    after = jnp.where(is_first, other[0:3], outer).astype(jnp.int32)
    relative = jnp.concatenate([before, ids[...], after], 1) - (start - 2 * BAND)
    pad = jnp.zeros((TILE - 3, height), jnp.int32)
    ids_col[...] = jnp.concatenate([relative, pad], 0).T
    here = lax.broadcasted_iota(jnp.int32, (1, height), 1) + (start - BAND)
    inside = jnp.where((here >= 0) & (here < total_cols), 1.0, 0.0)
    rows[...] = jnp.zeros_like(rows)
    wide = 128 + 2 * BAND
    for i in range(height // 128):
        at = 128 * i
        row = lax.broadcasted_iota(jnp.int32, (128, wide), 0) + at
        col = lax.broadcasted_iota(jnp.int32, (128, wide), 1) + at
        entry = jnp.where(col == row + BAND, 4.0, 0.0)
        for slot in range(3):
            entry = entry - jnp.where(col == ids_col[at : at + 128, slot : slot + 1], 1.0, 0.0)
        rows[at : at + 128, at : at + wide] = entry.astype(BF16)
    high[...] = jnp.zeros_like(high)
    low[...] = jnp.zeros_like(low)
    for i in range(col_count // 128):
        at = 128 * i
        col = lax.broadcasted_iota(jnp.int32, (128, wide), 0) + at
        row = lax.broadcasted_iota(jnp.int32, (128, wide), 1) + at
        entry = jnp.where(row == col + BAND, 4.0, 0.0)
        for slot in range(3):
            target = relative[slot : slot + 1, at : at + wide]
            entry = entry - jnp.where(col + 2 * BAND == target, 1.0, 0.0)
        own[...] = (entry * inside[:, at : at + wide]).astype(BF16)
        reach = slice(at, at + 128 + 4 * BAND)
        square = jnp.dot(own[...], rows[at : at + wide, reach], preferred_element_type=F32)
        high[at : at + 128, reach], low[at : at + 128, reach] = halves(square)


def forward(core, pair, own_high, own_low, far_high, far_low, part, wide):
    rows = wide.shape[0] // 2
    store_halves(wide, 0, pair[core[0]][:rows])
    store_halves(wide, rows, pair[1 - core[0]][:rows])
    part[...] = product(own_high, own_low, wide[:rows, :]) + product(far_high, far_low, wide[rows:, :])


def regularized(core, pair, edge, weight, m_high, m_low, near):
    reach = 2 * BAND
    rows = near.shape[0] - 2 * reach
    own, other = pair[core[0]][:rows], pair[1 - core[0]][:rows]
    is_first = core[0] == 0
    outer = edge[:reach, :]
    store_halves(near, 0, jnp.where(is_first, outer, other[rows - reach :]))
    store_halves(near, reach, own)
    store_halves(near, reach + rows, jnp.where(is_first, other[:reach], outer))
    return own, weight[...] * weight[...] * product(m_high, m_low, near[...])


def gathered(pieces, part):
    part[...] = summed(pieces)


def collect(core, part, pair, edge, weight, smooth, m_high, m_low, out, fresh, near):
    share = part.shape[0]
    out[:share, :] = part[...]
    own, new = regularized(core, pair, edge, weight, m_high, m_low, near)
    fresh[...] = new
    rows = [total(own * own), total(own * new), total(own * smooth[...])]
    out[share:, :] = jnp.concatenate([*rows, jnp.zeros((TILE - 3, own.shape[1]), F32)], 0)


def backward(every, field, fresh, old_image, old_smooth, old_way, old_scalars, high, low, moved, image, tail, smooth, way, scalars, wide):
    count = every.shape[0]
    share = every.shape[1] - TILE
    sums = every[0, share:, :]
    for k in range(1, count):
        sums = sums + every[k, share:, :]
    norm = sums[0:1]
    has_old = old_scalars[2:3, :] > 0.0
    ratio = jnp.where(has_old, norm / old_scalars[0:1, :], 0.0)
    square = jnp.zeros((TILE, every.shape[2]), F32)
    for k in range(0, count, 2):
        rows = slice(share * k, share * (k + 2))
        piece = jnp.concatenate([every[k, :share, :], every[k + 1, :share, :]], 0)
        piece = piece + ratio * old_image[rows, :]
        image[rows, :] = piece
        store_halves(wide, share * k, piece)
        for t in range(2 * share // TILE):
            block = piece[TILE * t : TILE * (t + 1)]
            square = square + block * block
    moved[...] = product(high, low, wide[...])
    put_rows(tail, [total(square)])
    smooth[...] = fresh[...] + ratio * old_smooth[...]
    way[...] = field[: way.shape[0], :] + ratio * old_way[...]
    reg_sq = sums[1:2] + ratio * (2.0 * sums[2:3] + ratio * old_scalars[1:2, :])
    put_rows(scalars, [norm, reg_sq, jnp.ones_like(norm)])


def spread(pieces, tail, out):
    share = pieces.shape[1]
    value, last = summed(pieces), tail[...]
    for k in range(out.shape[0]):
        out[k, :share, :] = value
        out[k, share:, :] = last


def spread_first(pieces, out):
    value = summed(pieces)
    for k in range(out.shape[0]):
        out[k] = value


def put_edge(core, rows, field, edge):
    reach = 2 * BAND
    edge[:reach, :] = jnp.where(core[0] == 0, field[:reach, :], field[rows - reach : rows, :])


def start_field(core, every, ids, field, edge):
    share = every.shape[1]
    rows, reach = field.shape[0] - TILE, edge.shape[0] - TILE
    for k in range(every.shape[0]):
        field[share * k : share * (k + 1), :] = every[k]
    put_edge(core, rows, field, edge)
    first, last = ids[:, :BAND].astype(F32), ids[:, ids.shape[1] - BAND :].astype(F32)
    field[rows:, :] = jnp.concatenate([first, last, jnp.zeros((TILE - 6, BAND), F32)], 0)
    sent = jnp.where(core[0] == 0, first, last)
    edge[reach:, :] = jnp.concatenate([sent, jnp.zeros((TILE - 3, BAND), F32)], 0)


def update(core, every, scalars, smooth, way, old_field, old_slip, field, edge, slip, kept):
    count = every.shape[0]
    share = every.shape[1] - TILE
    image_sq = every[0, share : share + 1, :]
    for k in range(1, count):
        image_sq = image_sq + every[k, share : share + 1, :]
    step = scalars[0:1, :] / (image_sq + scalars[1:2, :])
    for k in range(count):
        rows = slice(share * k, share * (k + 1))
        field[rows, :] = old_field[rows, :] - step * (every[k, :share, :] + smooth[rows, :])
    put_edge(core, field.shape[0], field, edge)
    slip[...] = old_slip[...] + step * way[...]
    put_rows(kept, [scalars[0:1, :], scalars[1:2, :], scalars[2:3, :], image_sq])


def last_sums(core, place, share_ref, image, pair, edge, weight, smooth, m_high, m_low, out, near):
    part = share_ref[...]
    share = part.shape[0]
    start = pl.multiple_of(place[0] * share, TILE)
    old = image[pl.ds(start, share), :]
    own, new = regularized(core, pair, edge, weight, m_high, m_low, near)
    rows = [total(own * own), total(own * new), total(own * smooth[...])]
    rows = [*rows, total(part * part), total(part * old)]
    first = jnp.concatenate([*rows, jnp.zeros((TILE - 5, own.shape[1]), F32)], 0)
    for k in range(out.shape[0]):
        out[k] = first


def last_spread(every, out):
    sums, pair = summed(every), every[0] + every[1]
    first = jnp.concatenate([pair[0:3], sums[3:]], 0)
    for k in range(out.shape[0]):
        out[k] = first


def last_update(every, kept, field, way, old_slip, slip):
    sums = summed(every)
    norm, old_norm, reg_sq, image_sq = sums[0:1], kept[0:1, :], kept[1:2, :], kept[3:4, :]
    ratio = norm / old_norm
    reg_sq = sums[1:2] + ratio * (2.0 * sums[2:3] + ratio * reg_sq)
    image_sq = sums[3:4] + ratio * (2.0 * sums[4:5] + ratio * image_sq)
    step = norm / (image_sq + reg_sq)
    slip[...] = old_slip[...] + step * (field[...] + ratio * way[...])


def exchanged(pieces, axis):
    return lax.all_to_all(pieces, axis, 0, 0, tiled=True)


def shards(green, data, neighbours, reg_weight):
    row_count, col_count = green.shape
    epochs = data.shape[1]
    n_obs, n_z, n_core = lax.axis_size(OBS), lax.axis_size(Z), lax.axis_size("c")
    n_patch = n_z * n_core
    core = lax.axis_index("c")
    piece = col_count // n_obs
    half = row_count // n_core
    reach = 2 * BAND
    weight = reg_weight[None]
    share = row_count // n_patch
    core_scalar = core.astype(jnp.int32)[None]
    row_scalar = lax.axis_index(("zh", "c", "zl")).astype(jnp.int32)[None]
    place_scalar = lax.axis_index(PATCH).astype(jnp.int32)[None]
    swap = [(0, 1), (1, 0)]
    outward = [(2 * z + 1, 2 * z + 2) for z in range(n_z - 1)]
    outward = outward + [(b, a) for a, b in outward]

    field_shape = ((col_count, epochs), F32)
    image_shape = ((row_count, epochs), F32)
    tail_shape = ((TILE, epochs), F32)
    wide = pltpu.VMEM((row_count, 2 * epochs), BF16)
    near = pltpu.VMEM((col_count + 2 * reach, 2 * epochs), BF16)

    back_matrix = ((col_count, row_count), BF16)
    matrix = ((half, col_count), BF16)
    moved, b_high, b_low, own_high, own_low, send = local_call(
        first_back,
        [field_shape, back_matrix, back_matrix, matrix, matrix, ((half, col_count), F32)],
        green, data, scalars=[core_scalar, place_scalar, row_scalar], scratch=[wide], share=share,
    )
    far = lax.ppermute(send, "c", swap)
    pieces = exchanged(moved.reshape(n_obs, piece, epochs), OBS)
    zero_tail = jnp.zeros((TILE, epochs), F32)
    zero_field = jnp.zeros((col_count, epochs), F32)
    spread_shape = ((n_obs, piece + TILE, epochs), F32)
    (out,) = local_call(spread_first, [((n_obs, piece, epochs), F32)], pieces)
    every = exchanged(out, OBS)
    edge_shape = ((reach, epochs), F32)
    long_field, long_edge = ((col_count + TILE, epochs), F32), ((reach + TILE, epochs), F32)
    field, edge = local_call(
        start_field, [long_field, long_edge], every, neighbours, scalars=[core_scalar]
    )
    far_high, far_low = local_call(split_other, [matrix, matrix], far)

    kept, slip, smooth, way = zero_tail, zero_field, zero_field, zero_field
    image = jnp.zeros((row_count, epochs), F32)
    for iteration in range(ITERS):
        edge = lax.ppermute(edge, PATCH, outward)
        pair = lax.all_gather(field, "c")
        (part,) = local_call(
            forward, [((half, epochs), F32)],
            pair, own_high, own_low, far_high, far_low,
            scalars=[core_scalar], scratch=[wide],
        )
        pieces = exchanged(part.reshape(2, half // 2, epochs), "zl")
        (part,) = local_call(gathered, [((half // 2, epochs), F32)], pieces)
        pieces = exchanged(part.reshape(n_z // 2, share, epochs), "zh")
        (part,) = local_call(gathered, [((share, epochs), F32)], pieces)
        if iteration == 0:
            m_matrix = ((col_count, col_count + 2 * reach), BF16)
            m_high, m_low = local_call(
                laplace_square, [m_matrix, m_matrix], pair, edge, neighbours,
                scalars=[core_scalar, place_scalar],
                n_patch=n_patch,
                scratch=[
                    pltpu.VMEM((col_count + reach, col_count + 2 * reach), BF16),
                    pltpu.VMEM((128, 128 + reach), BF16),
                    pltpu.VMEM((col_count + reach, TILE), jnp.int32),
                ],
            )
        penalty = (pair, edge, weight, smooth, m_high, m_low)
        if iteration + 1 == ITERS:
            shape = ((n_obs * n_core, TILE, epochs), F32)
            (out,) = local_call(
                last_sums, [shape], part, image, *penalty,
                scalars=[core_scalar, row_scalar], scratch=[near],
            )
            every = exchanged(out, (*OBS, "c"))
            (out,) = local_call(last_spread, [((n_z, TILE, epochs), F32)], every)
            (slip,) = local_call(
                last_update, [field_shape], exchanged(out, Z), kept, field, way, slip
            )
            return slip
        out, fresh = local_call(
            collect, [((share + TILE, epochs), F32), field_shape], part, *penalty,
            scalars=[core_scalar], scratch=[near],
        )
        every = lax.all_gather(lax.all_gather(out, "zl"), ("zh", "c"))
        every = every.reshape(n_patch, share + TILE, epochs)
        moved, image, tail, smooth, way, scalars = local_call(
            backward,
            [field_shape, image_shape, tail_shape, field_shape, field_shape, tail_shape],
            every, field, fresh, image, smooth, way, kept, b_high, b_low,
            scratch=[wide],
        )
        pieces = exchanged(moved.reshape(n_obs, piece, epochs), OBS)
        (out,) = local_call(spread, [spread_shape], pieces, tail)
        field, edge, slip, kept = local_call(
            update, [field_shape, edge_shape, field_shape, tail_shape],
            exchanged(out, OBS), scalars, smooth, way, field, slip,
            scalars=[core_scalar],
        )


def solution(mesh):
    split = Mesh(mesh.devices.reshape(4, 4, 8, 2, 2), (*OBS, *PATCH))
    in_specs = (P(OBS, PATCH), P(OBS, None), P(None, PATCH), P())

    return jax.shard_map(
        shards, mesh=split, in_specs=in_specs, out_specs=P(PATCH, None), check_vma=False
    )
```

```python
import functools

import jax
import jax.numpy as jnp
from jax import lax
from jax.experimental import pallas as pl
from jax.experimental.pallas import tpu as pltpu
from jax.sharding import Mesh
from jax.sharding import PartitionSpec as P

BAND = 128
ITERS = 3
OBS = ("x", "y")
Z = ("zh", "zl")
PATCH = (*Z, "c")
TILE = 8
F32, BF16 = jnp.float32, jnp.bfloat16


def local_call(body, outs, *args, scalars=(), scratch=(), mib=24, **options):
    vmem = pl.BlockSpec(memory_space=pltpu.VMEM)
    smem = pl.BlockSpec(memory_space=pltpu.SMEM)
    return pl.pallas_call(
        functools.partial(body, **options),
        out_shape=[jax.ShapeDtypeStruct(shape, kind) for shape, kind in outs],
        in_specs=[smem] * len(scalars) + [vmem] * len(args),
        out_specs=[vmem] * len(outs),
        scratch_shapes=list(scratch),
        compiler_params=pltpu.CompilerParams(vmem_limit_bytes=mib << 20),
    )(*scalars, *args)


def halves(x):
    high = x.astype(BF16)
    return high, (x - high.astype(F32)).astype(BF16)


def store_halves(ref, start, x):
    high, low = halves(x)
    ref[start : start + x.shape[0], : x.shape[1]] = high
    ref[start : start + x.shape[0], x.shape[1] :] = low


def product(high_ref, low_ref, wide):
    width = wide.shape[1] // 2
    both = jnp.dot(high_ref[...], wide, preferred_element_type=F32)
    both = both + jnp.dot(low_ref[...], wide, preferred_element_type=F32)
    return both[:, :width] + both[:, width:]


def total(x):
    return jnp.sum(x, axis=0, keepdims=True)


def put_rows(ref, rows):
    ref[...] = jnp.zeros_like(ref)
    for place, row in enumerate(rows):
        ref[place : place + 1, :] = row


def summed(pieces_ref):
    value = pieces_ref[0]
    for k in range(1, pieces_ref.shape[0]):
        value = value + pieces_ref[k]
    return value


def first_back(core, place, row, green, wide, moved, back_high, back_low, high, low, send, *, share):
    for k in range(green.shape[0] // 128):
        at = slice(128 * k, 128 * (k + 1))
        back_high[:, at], back_low[:, at] = halves(green[at, :].T)
    moved[...] = product(back_high, back_low, wide[...])
    half = send.shape[0]
    for z in range(0, half // share, 2):
        mine = []
        for k in (z, z + 1):
            start = pl.multiple_of((4 * (k // 2) + 2 * core[0] + k % 2) * share, TILE)
            mine.append(green[pl.ds(start, share), :])
            start = pl.multiple_of((4 * (k // 2) + 2 * (1 - core[0]) + k % 2) * share, TILE)
            send[share * k : share * (k + 1), :] = green[pl.ds(start, share), :]
        rows = slice(share * z, share * (z + 2))
        high[rows, :], low[rows, :] = halves(jnp.concatenate(mine, 0))


def split_other(other, high, low):
    high[...], low[...] = halves(other[...])


def laplace_square(core, block, pair, edge, ids, high, low, rows, own, ids_col, *, n_patch):
    col_count = ids.shape[1]
    height = rows.shape[0]
    total_cols = n_patch * col_count
    start = block[0] * col_count
    own_rows, edge_rows = pair.shape[1] - TILE, edge.shape[0] - TILE
    other = pair[1 - core[0]][own_rows:]
    outer = edge[edge_rows : edge_rows + 3, :]
    is_first = core[0] == 0
    before = jnp.where(is_first, outer, other[3:6]).astype(jnp.int32)
    after = jnp.where(is_first, other[0:3], outer).astype(jnp.int32)
    relative = jnp.concatenate([before, ids[...], after], 1) - (start - 2 * BAND)
    pad = jnp.zeros((TILE - 3, height), jnp.int32)
    ids_col[...] = jnp.concatenate([relative, pad], 0).T
    here = lax.broadcasted_iota(jnp.int32, (1, height), 1) + (start - BAND)
    inside = jnp.where((here >= 0) & (here < total_cols), 1.0, 0.0)
    rows[...] = jnp.zeros_like(rows)
    wide = 128 + 2 * BAND
    for i in range(height // 128):
        at = 128 * i
        row = lax.broadcasted_iota(jnp.int32, (128, wide), 0) + at
        col = lax.broadcasted_iota(jnp.int32, (128, wide), 1) + at
        entry = jnp.where(col == row + BAND, 4.0, 0.0)
        for slot in range(3):
            entry = entry - jnp.where(col == ids_col[at : at + 128, slot : slot + 1], 1.0, 0.0)
        rows[at : at + 128, at : at + wide] = entry.astype(BF16)
    high[...] = jnp.zeros_like(high)
    low[...] = jnp.zeros_like(low)
    for i in range(col_count // 128):
        at = 128 * i
        col = lax.broadcasted_iota(jnp.int32, (128, wide), 0) + at
        row = lax.broadcasted_iota(jnp.int32, (128, wide), 1) + at
        entry = jnp.where(row == col + BAND, 4.0, 0.0)
        for slot in range(3):
            target = relative[slot : slot + 1, at : at + wide]
            entry = entry - jnp.where(col + 2 * BAND == target, 1.0, 0.0)
        own[...] = (entry * inside[:, at : at + wide]).astype(BF16)
        reach = slice(at, at + 128 + 4 * BAND)
        square = jnp.dot(own[...], rows[at : at + wide, reach], preferred_element_type=F32)
        high[at : at + 128, reach], low[at : at + 128, reach] = halves(square)


def forward(core, pair, own_high, own_low, far_high, far_low, part, wide):
    rows = wide.shape[0] // 2
    store_halves(wide, 0, pair[core[0]][:rows])
    store_halves(wide, rows, pair[1 - core[0]][:rows])
    part[...] = product(own_high, own_low, wide[:rows, :]) + product(far_high, far_low, wide[rows:, :])


def regularized(core, pair, edge, weight, m_high, m_low, near):
    reach = 2 * BAND
    rows = near.shape[0] - 2 * reach
    own, other = pair[core[0]][:rows], pair[1 - core[0]][:rows]
    is_first = core[0] == 0
    outer = edge[:reach, :]
    store_halves(near, 0, jnp.where(is_first, outer, other[rows - reach :]))
    store_halves(near, reach, own)
    store_halves(near, reach + rows, jnp.where(is_first, other[:reach], outer))
    return own, weight[...] * weight[...] * product(m_high, m_low, near[...])


def gathered(pieces, part):
    part[...] = summed(pieces)


def collect(core, part, pair, edge, weight, smooth, m_high, m_low, out, fresh, near):
    share = part.shape[0]
    out[:share, :] = part[...]
    own, new = regularized(core, pair, edge, weight, m_high, m_low, near)
    fresh[...] = new
    rows = [total(own * own), total(own * new), total(own * smooth[...])]
    out[share:, :] = jnp.concatenate([*rows, jnp.zeros((TILE - 3, own.shape[1]), F32)], 0)


def backward(every, field, fresh, old_image, old_smooth, old_way, old_scalars, high, low, moved, image, tail, smooth, way, scalars, wide):
    count = every.shape[0]
    share = every.shape[1] - TILE
    sums = every[0, share:, :]
    for k in range(1, count):
        sums = sums + every[k, share:, :]
    norm = sums[0:1]
    has_old = old_scalars[2:3, :] > 0.0
    ratio = jnp.where(has_old, norm / old_scalars[0:1, :], 0.0)
    square = jnp.zeros((TILE, every.shape[2]), F32)
    for k in range(0, count, 2):
        rows = slice(share * k, share * (k + 2))
        piece = jnp.concatenate([every[k, :share, :], every[k + 1, :share, :]], 0)
        piece = piece + ratio * old_image[rows, :]
        image[rows, :] = piece
        store_halves(wide, share * k, piece)
        for t in range(2 * share // TILE):
            block = piece[TILE * t : TILE * (t + 1)]
            square = square + block * block
    moved[...] = product(high, low, wide[...])
    put_rows(tail, [total(square)])
    smooth[...] = fresh[...] + ratio * old_smooth[...]
    way[...] = field[: way.shape[0], :] + ratio * old_way[...]
    reg_sq = sums[1:2] + ratio * (2.0 * sums[2:3] + ratio * old_scalars[1:2, :])
    put_rows(scalars, [norm, reg_sq, jnp.ones_like(norm)])


def spread(pieces, tail, out):
    share = pieces.shape[1]
    value, last = summed(pieces), tail[...]
    for k in range(out.shape[0]):
        out[k, :share, :] = value
        out[k, share:, :] = last


def spread_first(pieces, out):
    value = summed(pieces)
    for k in range(out.shape[0]):
        out[k] = value


def put_edge(core, rows, field, edge):
    reach = 2 * BAND
    edge[:reach, :] = jnp.where(core[0] == 0, field[:reach, :], field[rows - reach : rows, :])


def start_field(core, every, ids, field, edge):
    share = every.shape[1]
    rows, reach = field.shape[0] - TILE, edge.shape[0] - TILE
    for k in range(every.shape[0]):
        field[share * k : share * (k + 1), :] = every[k]
    put_edge(core, rows, field, edge)
    first, last = ids[:, :BAND].astype(F32), ids[:, ids.shape[1] - BAND :].astype(F32)
    field[rows:, :] = jnp.concatenate([first, last, jnp.zeros((TILE - 6, BAND), F32)], 0)
    sent = jnp.where(core[0] == 0, first, last)
    edge[reach:, :] = jnp.concatenate([sent, jnp.zeros((TILE - 3, BAND), F32)], 0)


def update(core, every, scalars, smooth, way, old_field, old_slip, field, edge, slip, kept):
    count = every.shape[0]
    share = every.shape[1] - TILE
    image_sq = every[0, share : share + 1, :]
    for k in range(1, count):
        image_sq = image_sq + every[k, share : share + 1, :]
    step = scalars[0:1, :] / (image_sq + scalars[1:2, :])
    for k in range(count):
        rows = slice(share * k, share * (k + 1))
        field[rows, :] = old_field[rows, :] - step * (every[k, :share, :] + smooth[rows, :])
    put_edge(core, field.shape[0], field, edge)
    slip[...] = old_slip[...] + step * way[...]
    put_rows(kept, [scalars[0:1, :], scalars[1:2, :], scalars[2:3, :], image_sq])


def last_sums(core, place, share_ref, image, pair, edge, weight, smooth, m_high, m_low, out, near):
    part = share_ref[...]
    share = part.shape[0]
    start = pl.multiple_of(place[0] * share, TILE)
    old = image[pl.ds(start, share), :]
    own, new = regularized(core, pair, edge, weight, m_high, m_low, near)
    rows = [total(own * own), total(own * new), total(own * smooth[...])]
    rows = [*rows, total(part * part), total(part * old)]
    first = jnp.concatenate([*rows, jnp.zeros((TILE - 5, own.shape[1]), F32)], 0)
    for k in range(out.shape[0]):
        out[k] = first


def last_spread(every, out):
    sums, pair = summed(every), every[0] + every[1]
    first = jnp.concatenate([pair[0:3], sums[3:]], 0)
    for k in range(out.shape[0]):
        out[k] = first


def last_update(every, kept, field, way, old_slip, slip):
    sums = summed(every)
    norm, old_norm, reg_sq, image_sq = sums[0:1], kept[0:1, :], kept[1:2, :], kept[3:4, :]
    ratio = norm / old_norm
    reg_sq = sums[1:2] + ratio * (2.0 * sums[2:3] + ratio * reg_sq)
    image_sq = sums[3:4] + ratio * (2.0 * sums[4:5] + ratio * image_sq)
    step = norm / (image_sq + reg_sq)
    slip[...] = old_slip[...] + step * (field[...] + ratio * way[...])


def exchanged(pieces, axis):
    return lax.all_to_all(pieces, axis, 0, 0, tiled=True)


def shards(green, data, neighbours, reg_weight):
    row_count, col_count = green.shape
    epochs = data.shape[1]
    n_obs, n_z, n_core = lax.axis_size(OBS), lax.axis_size(Z), lax.axis_size("c")
    n_patch = n_z * n_core
    core = lax.axis_index("c")
    piece = col_count // n_obs
    half = row_count // n_core
    reach = 2 * BAND
    weight = reg_weight[None]
    share = row_count // n_patch
    core_scalar = core.astype(jnp.int32)[None]
    row_scalar = lax.axis_index(("zh", "c", "zl")).astype(jnp.int32)[None]
    place_scalar = lax.axis_index(PATCH).astype(jnp.int32)[None]
    swap = [(0, 1), (1, 0)]
    outward = [(2 * z + 1, 2 * z + 2) for z in range(n_z - 1)]
    outward = outward + [(b, a) for a, b in outward]

    field_shape = ((col_count, epochs), F32)
    image_shape = ((row_count, epochs), F32)
    tail_shape = ((TILE, epochs), F32)
    wide = pltpu.VMEM((row_count, 2 * epochs), BF16)
    near = pltpu.VMEM((col_count + 2 * reach, 2 * epochs), BF16)

    back_matrix = ((col_count, row_count), BF16)
    matrix = ((half, col_count), BF16)
    rounded = lax.reduce_precision(data, 8, 7)
    data_wide = jnp.concatenate([rounded, data - rounded], 1).astype(BF16)
    moved, b_high, b_low, own_high, own_low, send = local_call(
        first_back,
        [field_shape, back_matrix, back_matrix, matrix, matrix, ((half, col_count), F32)],
        green, data_wide, scalars=[core_scalar, place_scalar, row_scalar], share=share,
    )
    far = lax.ppermute(send, "c", swap)
    pieces = exchanged(moved.reshape(n_obs, piece, epochs), OBS)
    zero_tail = jnp.zeros((TILE, epochs), F32)
    zero_field = jnp.zeros((col_count, epochs), F32)
    spread_shape = ((n_obs, piece + TILE, epochs), F32)
    (out,) = local_call(spread_first, [((n_obs, piece, epochs), F32)], pieces)
    every = exchanged(out, OBS)
    edge_shape = ((reach, epochs), F32)
    long_field, long_edge = ((col_count + TILE, epochs), F32), ((reach + TILE, epochs), F32)
    field, edge = local_call(
        start_field, [long_field, long_edge], every, neighbours, scalars=[core_scalar]
    )
    far_high, far_low = local_call(split_other, [matrix, matrix], far)

    kept, slip, smooth, way = zero_tail, zero_field, zero_field, zero_field
    image = jnp.zeros((row_count, epochs), F32)
    for iteration in range(ITERS):
        edge = lax.ppermute(edge, PATCH, outward)
        pair = lax.all_gather(field, "c")
        (part,) = local_call(
            forward, [((half, epochs), F32)],
            pair, own_high, own_low, far_high, far_low,
            scalars=[core_scalar], scratch=[wide],
        )
        pieces = exchanged(part.reshape(n_z, share, epochs), Z)
        (part,) = local_call(gathered, [((share, epochs), F32)], pieces)
        if iteration == 0:
            m_matrix = ((col_count, col_count + 2 * reach), BF16)
            m_high, m_low = local_call(
                laplace_square, [m_matrix, m_matrix], pair, edge, neighbours,
                scalars=[core_scalar, place_scalar],
                n_patch=n_patch,
                scratch=[
                    pltpu.VMEM((col_count + reach, col_count + 2 * reach), BF16),
                    pltpu.VMEM((128, 128 + reach), BF16),
                    pltpu.VMEM((col_count + reach, TILE), jnp.int32),
                ],
            )
        penalty = (pair, edge, weight, smooth, m_high, m_low)
        if iteration + 1 == ITERS:
            shape = ((n_obs * n_core, TILE, epochs), F32)
            (out,) = local_call(
                last_sums, [shape], part, image, *penalty,
                scalars=[core_scalar, row_scalar], scratch=[near],
            )
            every = exchanged(out, (*OBS, "c"))
            (out,) = local_call(last_spread, [((n_z, TILE, epochs), F32)], every)
            (slip,) = local_call(
                last_update, [field_shape], exchanged(out, Z), kept, field, way, slip
            )
            return slip
        out, fresh = local_call(
            collect, [((share + TILE, epochs), F32), field_shape], part, *penalty,
            scalars=[core_scalar], scratch=[near],
        )
        every = lax.all_gather(lax.all_gather(out, "zl"), ("zh", "c"))
        every = every.reshape(n_patch, share + TILE, epochs)
        moved, image, tail, smooth, way, scalars = local_call(
            backward,
            [field_shape, image_shape, tail_shape, field_shape, field_shape, tail_shape],
            every, field, fresh, image, smooth, way, kept, b_high, b_low,
            scratch=[wide],
        )
        pieces = exchanged(moved.reshape(n_obs, piece, epochs), OBS)
        (out,) = local_call(spread, [spread_shape], pieces, tail)
        field, edge, slip, kept = local_call(
            update, [field_shape, edge_shape, field_shape, tail_shape],
            exchanged(out, OBS), scalars, smooth, way, field, slip,
            scalars=[core_scalar],
        )


def solution(mesh):
    split = Mesh(mesh.devices.reshape(4, 4, 8, 2, 2), (*OBS, *PATCH))
    in_specs = (P(OBS, PATCH), P(OBS, None), P(None, PATCH), P())

    return jax.shard_map(
        shards, mesh=split, in_specs=in_specs, out_specs=P(PATCH, None), check_vma=False
    )
```

```python
import functools

import jax
import jax.numpy as jnp
from jax import lax
from jax.experimental import pallas as pl
from jax.experimental.pallas import tpu as pltpu
from jax.sharding import Mesh
from jax.sharding import PartitionSpec as P

BAND = 128
ITERS = 3
OBS = ("x", "y")
Z = ("zh", "zl")
PATCH = (*Z, "c")
TILE = 8
F32, BF16 = jnp.float32, jnp.bfloat16


def local_call(body, outs, *args, scalars=(), scratch=(), mib=24, **options):
    vmem = pl.BlockSpec(memory_space=pltpu.VMEM)
    smem = pl.BlockSpec(memory_space=pltpu.SMEM)
    return pl.pallas_call(
        functools.partial(body, **options),
        out_shape=[jax.ShapeDtypeStruct(shape, kind) for shape, kind in outs],
        in_specs=[smem] * len(scalars) + [vmem] * len(args),
        out_specs=[vmem] * len(outs),
        scratch_shapes=list(scratch),
        compiler_params=pltpu.CompilerParams(vmem_limit_bytes=mib << 20),
    )(*scalars, *args)


def halves(x):
    high = x.astype(BF16)
    return high, (x - high.astype(F32)).astype(BF16)


def store_halves(ref, start, x):
    high, low = halves(x)
    ref[start : start + x.shape[0], : x.shape[1]] = high
    ref[start : start + x.shape[0], x.shape[1] :] = low


def product(high_ref, low_ref, wide):
    width = wide.shape[1] // 2
    both = jnp.dot(high_ref[...], wide, preferred_element_type=F32)
    both = both + jnp.dot(low_ref[...], wide, preferred_element_type=F32)
    return both[:, :width] + both[:, width:]


def total(x):
    return jnp.sum(x, axis=0, keepdims=True)


def put_rows(ref, rows):
    ref[...] = jnp.zeros_like(ref)
    for place, row in enumerate(rows):
        ref[place : place + 1, :] = row


def summed(pieces_ref):
    value = pieces_ref[0]
    for k in range(1, pieces_ref.shape[0]):
        value = value + pieces_ref[k]
    return value


def first_back(core, place, row, green, data, moved, back_high, back_low, high, low, send, wide, *, share):
    for k in range(green.shape[0] // 128):
        at = slice(128 * k, 128 * (k + 1))
        back_high[:, at], back_low[:, at] = halves(green[at, :].T)
    store_halves(wide, 0, data[...])
    moved[...] = product(back_high, back_low, wide[...])
    half = send.shape[0]
    for z in range(0, half // share, 2):
        mine = []
        for k in (z, z + 1):
            start = pl.multiple_of((4 * (k // 2) + 2 * core[0] + k % 2) * share, TILE)
            mine.append(green[pl.ds(start, share), :])
            start = pl.multiple_of((4 * (k // 2) + 2 * (1 - core[0]) + k % 2) * share, TILE)
            send[share * k : share * (k + 1), :] = green[pl.ds(start, share), :]
        rows = slice(share * z, share * (z + 2))
        high[rows, :], low[rows, :] = halves(jnp.concatenate(mine, 0))


def split_other(other, high, low):
    high[...], low[...] = halves(other[...])


def laplace_square(core, block, pair, edge, ids, high, low, rows, own, ids_col, *, n_patch):
    col_count = ids.shape[1]
    height = rows.shape[0]
    total_cols = n_patch * col_count
    start = block[0] * col_count
    own_rows, edge_rows = pair.shape[1] - TILE, edge.shape[0] - TILE
    other = pair[1 - core[0]][own_rows:]
    outer = edge[edge_rows : edge_rows + 3, :]
    is_first = core[0] == 0
    before = jnp.where(is_first, outer, other[3:6]).astype(jnp.int32)
    after = jnp.where(is_first, other[0:3], outer).astype(jnp.int32)
    relative = jnp.concatenate([before, ids[...], after], 1) - (start - 2 * BAND)
    pad = jnp.zeros((TILE - 3, height), jnp.int32)
    ids_col[...] = jnp.concatenate([relative, pad], 0).T
    here = lax.broadcasted_iota(jnp.int32, (1, height), 1) + (start - BAND)
    inside = jnp.where((here >= 0) & (here < total_cols), 1.0, 0.0)
    rows[...] = jnp.zeros_like(rows)
    wide = 128 + 2 * BAND
    for i in range(height // 128):
        at = 128 * i
        row = lax.broadcasted_iota(jnp.int32, (128, wide), 0) + at
        col = lax.broadcasted_iota(jnp.int32, (128, wide), 1) + at
        entry = jnp.where(col == row + BAND, 4.0, 0.0)
        for slot in range(3):
            entry = entry - jnp.where(col == ids_col[at : at + 128, slot : slot + 1], 1.0, 0.0)
        rows[at : at + 128, at : at + wide] = entry.astype(BF16)
    high[...] = jnp.zeros_like(high)
    low[...] = jnp.zeros_like(low)
    for i in range(col_count // 128):
        at = 128 * i
        col = lax.broadcasted_iota(jnp.int32, (128, wide), 0) + at
        row = lax.broadcasted_iota(jnp.int32, (128, wide), 1) + at
        entry = jnp.where(row == col + BAND, 4.0, 0.0)
        for slot in range(3):
            target = relative[slot : slot + 1, at : at + wide]
            entry = entry - jnp.where(col + 2 * BAND == target, 1.0, 0.0)
        own[...] = (entry * inside[:, at : at + wide]).astype(BF16)
        reach = slice(at, at + 128 + 4 * BAND)
        square = jnp.dot(own[...], rows[at : at + wide, reach], preferred_element_type=F32)
        high[at : at + 128, reach], low[at : at + 128, reach] = halves(square)


def forward(core, pair, own_high, own_low, far_high, far_low, part, wide):
    rows = wide.shape[0] // 2
    store_halves(wide, 0, pair[core[0]][:rows])
    store_halves(wide, rows, pair[1 - core[0]][:rows])
    part[...] = product(own_high, own_low, wide[:rows, :]) + product(far_high, far_low, wide[rows:, :])


def regularized(core, pair, edge, weight, m_high, m_low, near):
    reach = 2 * BAND
    rows = near.shape[0] - 2 * reach
    own, other = pair[core[0]][:rows], pair[1 - core[0]][:rows]
    is_first = core[0] == 0
    outer = edge[:reach, :]
    store_halves(near, 0, jnp.where(is_first, outer, other[rows - reach :]))
    store_halves(near, reach, own)
    store_halves(near, reach + rows, jnp.where(is_first, other[:reach], outer))
    return own, weight[...] * weight[...] * product(m_high, m_low, near[...])


def gathered(pieces, part):
    part[...] = summed(pieces)


def collect(core, part, pair, edge, weight, smooth, m_high, m_low, out, fresh, near):
    share = part.shape[0]
    out[:share, :] = part[...]
    own, new = regularized(core, pair, edge, weight, m_high, m_low, near)
    fresh[...] = new
    rows = [total(own * own), total(own * new), total(own * smooth[...])]
    out[share:, :] = jnp.concatenate([*rows, jnp.zeros((TILE - 3, own.shape[1]), F32)], 0)


def merged(pair, out):
    share = pair.shape[1] - TILE
    out[:share, :] = pair[0, :share, :]
    out[share : 2 * share, :] = pair[1, :share, :]
    out[2 * share :, :] = pair[0, share:, :] + pair[1, share:, :]


def backward(every, field, fresh, old_image, old_smooth, old_way, old_scalars, high, low, moved, image, tail, smooth, way, scalars, wide):
    count = every.shape[0]
    share = every.shape[1] - TILE
    sums = every[0, share:, :]
    for k in range(1, count):
        sums = sums + every[k, share:, :]
    norm = sums[0:1]
    has_old = old_scalars[2:3, :] > 0.0
    ratio = jnp.where(has_old, norm / old_scalars[0:1, :], 0.0)
    square = jnp.zeros((TILE, every.shape[2]), F32)
    for k in range(count):
        rows = slice(share * k, share * (k + 1))
        piece = every[k, :share, :] + ratio * old_image[rows, :]
        image[rows, :] = piece
        store_halves(wide, share * k, piece)
        for t in range(share // TILE):
            block = piece[TILE * t : TILE * (t + 1)]
            square = square + block * block
    moved[...] = product(high, low, wide[...])
    put_rows(tail, [total(square)])
    smooth[...] = fresh[...] + ratio * old_smooth[...]
    way[...] = field[: way.shape[0], :] + ratio * old_way[...]
    reg_sq = sums[1:2] + ratio * (2.0 * sums[2:3] + ratio * old_scalars[1:2, :])
    put_rows(scalars, [norm, reg_sq, jnp.ones_like(norm)])


def spread(pieces, tail, out):
    share = pieces.shape[1]
    value, last = summed(pieces), tail[...]
    for k in range(out.shape[0]):
        out[k, :share, :] = value
        out[k, share:, :] = last


def spread_first(pieces, out):
    value = summed(pieces)
    for k in range(out.shape[0]):
        out[k] = value


def put_edge(core, rows, field, edge):
    reach = 2 * BAND
    edge[:reach, :] = jnp.where(core[0] == 0, field[:reach, :], field[rows - reach : rows, :])


def start_field(core, every, ids, field, edge):
    share = every.shape[1]
    rows, reach = field.shape[0] - TILE, edge.shape[0] - TILE
    for k in range(every.shape[0]):
        field[share * k : share * (k + 1), :] = every[k]
    put_edge(core, rows, field, edge)
    first, last = ids[:, :BAND].astype(F32), ids[:, ids.shape[1] - BAND :].astype(F32)
    field[rows:, :] = jnp.concatenate([first, last, jnp.zeros((TILE - 6, BAND), F32)], 0)
    sent = jnp.where(core[0] == 0, first, last)
    edge[reach:, :] = jnp.concatenate([sent, jnp.zeros((TILE - 3, BAND), F32)], 0)


def update(core, every, scalars, smooth, way, old_field, old_slip, field, edge, slip, kept):
    count = every.shape[0]
    share = every.shape[1] - TILE
    image_sq = every[0, share : share + 1, :]
    for k in range(1, count):
        image_sq = image_sq + every[k, share : share + 1, :]
    step = scalars[0:1, :] / (image_sq + scalars[1:2, :])
    for k in range(count):
        rows = slice(share * k, share * (k + 1))
        field[rows, :] = old_field[rows, :] - step * (every[k, :share, :] + smooth[rows, :])
    put_edge(core, field.shape[0], field, edge)
    slip[...] = old_slip[...] + step * way[...]
    put_rows(kept, [scalars[0:1, :], scalars[1:2, :], scalars[2:3, :], image_sq])


def last_sums(core, place, share_ref, image, pair, edge, weight, smooth, m_high, m_low, out, near):
    part = share_ref[...]
    share = part.shape[0]
    start = pl.multiple_of(place[0] * share, TILE)
    old = image[pl.ds(start, share), :]
    own, new = regularized(core, pair, edge, weight, m_high, m_low, near)
    rows = [total(own * own), total(own * new), total(own * smooth[...])]
    rows = [*rows, total(part * part), total(part * old)]
    first = jnp.concatenate([*rows, jnp.zeros((TILE - 5, own.shape[1]), F32)], 0)
    for k in range(out.shape[0]):
        out[k] = first


def last_spread(every, out):
    sums, pair = summed(every), every[0] + every[1]
    first = jnp.concatenate([pair[0:3], sums[3:]], 0)
    for k in range(out.shape[0]):
        out[k] = first


def last_update(every, kept, field, way, old_slip, slip):
    sums = summed(every)
    norm, old_norm, reg_sq, image_sq = sums[0:1], kept[0:1, :], kept[1:2, :], kept[3:4, :]
    ratio = norm / old_norm
    reg_sq = sums[1:2] + ratio * (2.0 * sums[2:3] + ratio * reg_sq)
    image_sq = sums[3:4] + ratio * (2.0 * sums[4:5] + ratio * image_sq)
    step = norm / (image_sq + reg_sq)
    slip[...] = old_slip[...] + step * (field[...] + ratio * way[...])


def exchanged(pieces, axis):
    return lax.all_to_all(pieces, axis, 0, 0, tiled=True)


def shards(green, data, neighbours, reg_weight):
    row_count, col_count = green.shape
    epochs = data.shape[1]
    n_obs, n_z, n_core = lax.axis_size(OBS), lax.axis_size(Z), lax.axis_size("c")
    n_patch = n_z * n_core
    core = lax.axis_index("c")
    piece = col_count // n_obs
    half = row_count // n_core
    reach = 2 * BAND
    weight = reg_weight[None]
    share = row_count // n_patch
    core_scalar = core.astype(jnp.int32)[None]
    row_scalar = lax.axis_index(("zh", "c", "zl")).astype(jnp.int32)[None]
    place_scalar = lax.axis_index(PATCH).astype(jnp.int32)[None]
    swap = [(0, 1), (1, 0)]
    outward = [(2 * z + 1, 2 * z + 2) for z in range(n_z - 1)]
    outward = outward + [(b, a) for a, b in outward]

    field_shape = ((col_count, epochs), F32)
    image_shape = ((row_count, epochs), F32)
    tail_shape = ((TILE, epochs), F32)
    wide = pltpu.VMEM((row_count, 2 * epochs), BF16)
    near = pltpu.VMEM((col_count + 2 * reach, 2 * epochs), BF16)

    back_matrix = ((col_count, row_count), BF16)
    matrix = ((half, col_count), BF16)
    moved, b_high, b_low, own_high, own_low, send = local_call(
        first_back,
        [field_shape, back_matrix, back_matrix, matrix, matrix, ((half, col_count), F32)],
        green, data, scalars=[core_scalar, place_scalar, row_scalar], scratch=[wide], share=share,
    )
    far = lax.ppermute(send, "c", swap)
    pieces = exchanged(moved.reshape(n_obs, piece, epochs), OBS)
    zero_tail = jnp.zeros((TILE, epochs), F32)
    zero_field = jnp.zeros((col_count, epochs), F32)
    spread_shape = ((n_obs, piece + TILE, epochs), F32)
    (out,) = local_call(spread_first, [((n_obs, piece, epochs), F32)], pieces)
    every = exchanged(out, OBS)
    edge_shape = ((reach, epochs), F32)
    long_field, long_edge = ((col_count + TILE, epochs), F32), ((reach + TILE, epochs), F32)
    field, edge = local_call(
        start_field, [long_field, long_edge], every, neighbours, scalars=[core_scalar]
    )
    far_high, far_low = local_call(split_other, [matrix, matrix], far)

    kept, slip, smooth, way = zero_tail, zero_field, zero_field, zero_field
    image = jnp.zeros((row_count, epochs), F32)
    for iteration in range(ITERS):
        edge = lax.ppermute(edge, PATCH, outward)
        pair = lax.all_gather(field, "c")
        (part,) = local_call(
            forward, [((half, epochs), F32)],
            pair, own_high, own_low, far_high, far_low,
            scalars=[core_scalar], scratch=[wide],
        )
        pieces = exchanged(part.reshape(n_z, share, epochs), Z)
        (part,) = local_call(gathered, [((share, epochs), F32)], pieces)
        if iteration == 0:
            m_matrix = ((col_count, col_count + 2 * reach), BF16)
            m_high, m_low = local_call(
                laplace_square, [m_matrix, m_matrix], pair, edge, neighbours,
                scalars=[core_scalar, place_scalar],
                n_patch=n_patch,
                scratch=[
                    pltpu.VMEM((col_count + reach, col_count + 2 * reach), BF16),
                    pltpu.VMEM((128, 128 + reach), BF16),
                    pltpu.VMEM((col_count + reach, TILE), jnp.int32),
                ],
            )
        penalty = (pair, edge, weight, smooth, m_high, m_low)
        if iteration + 1 == ITERS:
            shape = ((n_obs * n_core, TILE, epochs), F32)
            (out,) = local_call(
                last_sums, [shape], part, image, *penalty,
                scalars=[core_scalar, row_scalar], scratch=[near],
            )
            every = exchanged(out, (*OBS, "c"))
            (out,) = local_call(last_spread, [((n_z, TILE, epochs), F32)], every)
            (slip,) = local_call(
                last_update, [field_shape], exchanged(out, Z), kept, field, way, slip
            )
            return slip
        out, fresh = local_call(
            collect, [((share + TILE, epochs), F32), field_shape], part, *penalty,
            scalars=[core_scalar], scratch=[near],
        )
        (out,) = local_call(merged, [((2 * share + TILE, epochs), F32)], lax.all_gather(out, "zl"))
        every = lax.all_gather(out, ("zh", "c"))
        moved, image, tail, smooth, way, scalars = local_call(
            backward,
            [field_shape, image_shape, tail_shape, field_shape, field_shape, tail_shape],
            every, field, fresh, image, smooth, way, kept, b_high, b_low,
            scratch=[wide],
        )
        pieces = exchanged(moved.reshape(n_obs, piece, epochs), OBS)
        (out,) = local_call(spread, [spread_shape], pieces, tail)
        field, edge, slip, kept = local_call(
            update, [field_shape, edge_shape, field_shape, tail_shape],
            exchanged(out, OBS), scalars, smooth, way, field, slip,
            scalars=[core_scalar],
        )


def solution(mesh):
    split = Mesh(mesh.devices.reshape(4, 4, 8, 2, 2), (*OBS, *PATCH))
    in_specs = (P(OBS, PATCH), P(OBS, None), P(None, PATCH), P())

    return jax.shard_map(
        shards, mesh=split, in_specs=in_specs, out_specs=P(PATCH, None), check_vma=False
    )
```
